16 devices in a mesh: data: 16 (over z, y, x, core).
Axes of the slice: x: 2, y: 2, z: 2, core: 2. Of those that a mesh axis runs over, the one named last changes fastest.
Arguments:
- q_in: bfloat16 [8192, 384], P('data')
- d_in: bfloat16 [2, 8192, 384], P(None, 'data')
- temperature: float32 [], replicated
- q_w1: bfloat16 [2, 384, 1536], replicated
- q_w2: bfloat16 [2, 1536, 384], replicated
- q_proj: bfloat16 [384, 384], replicated
- d_w1: bfloat16 [2, 384, 1536], replicated
- d_w2: bfloat16 [2, 1536, 384], replicated
- d_proj: bfloat16 [384, 384], replicated
Outputs:
- output 1: float32 [], replicated
- output 2: float32 [2, 384, 1536], replicated
- output 3: float32 [2, 1536, 384], replicated
- output 4: float32 [384, 384], replicated
- output 5: float32 [2, 384, 1536], replicated
- output 6: float32 [2, 1536, 384], replicated
- output 7: float32 [384, 384], replicated
All inputs are finite; a program needn't handle non-finite values.
Results may differ from the reference program's by a relative error of at most 0.00545337.
Values are sent between devices in bfloat16 or wider.
A program may use at most 1 GiB of HBM per device.

```python
import math
import jax
import jax.numpy as jnp
from jax import lax

GLOBAL_BATCH = 8192
SHARD_ROWS = 512
HIDDEN = 384
FFN_WIDTH = 1536
REPR_DIM = 384


def setup_inputs(seed: int = 0) -> dict:
    key_list = jax.random.split(jax.random.key(seed), 9)
    sharpness = 0.8 * math.sqrt(2.0 * math.log(2.0 * GLOBAL_BATCH))
    tau_base = 2.0 * math.sqrt(REPR_DIM) / sharpness

    def weight(w_key, w_shape, fan_in):
        return (jax.random.normal(w_key, w_shape, jnp.float32) * fan_in ** -0.5).astype(jnp.bfloat16)

    return dict(
        q_in=jax.random.normal(key_list[0], (GLOBAL_BATCH, HIDDEN), jnp.float32).astype(jnp.bfloat16),
        d_in=jax.random.normal(key_list[1], (2, GLOBAL_BATCH, HIDDEN), jnp.float32).astype(jnp.bfloat16),
        temperature=tau_base * jax.random.uniform(key_list[2], (), jnp.float32, 0.8, 1.25),
        q_w1=weight(key_list[3], (2, HIDDEN, FFN_WIDTH), HIDDEN),
        q_w2=weight(key_list[4], (2, FFN_WIDTH, HIDDEN), FFN_WIDTH),
        q_proj=weight(key_list[5], (HIDDEN, REPR_DIM), HIDDEN),
        d_w1=weight(key_list[6], (2, HIDDEN, FFN_WIDTH), HIDDEN),
        d_w2=weight(key_list[7], (2, FFN_WIDTH, HIDDEN), FFN_WIDTH),
        d_proj=weight(key_list[8], (HIDDEN, REPR_DIM), HIDDEN),
    )


def tower_forward(row_block, w_one, w_two, w_proj):
    hidden = row_block
    saved = []
    for layer in range(2):
        pre_act = jnp.dot(hidden, w_one[layer], preferred_element_type=jnp.float32)
        act_bf = jax.nn.gelu(pre_act).astype(jnp.bfloat16)
        saved.append((hidden, pre_act, act_bf))
        hidden = (hidden.astype(jnp.float32) + jnp.dot(act_bf, w_two[layer], preferred_element_type=jnp.float32)).astype(jnp.bfloat16)
    out_reps = jnp.dot(hidden, w_proj, preferred_element_type=jnp.float32).astype(jnp.bfloat16)
    return out_reps, hidden, saved


def tower_backward(upstream, w_one, w_two, w_proj, hidden, saved):
    g_proj = jnp.dot(hidden.T, upstream, preferred_element_type=jnp.float32)
    resid_grad = jnp.dot(upstream, w_proj.T, preferred_element_type=jnp.float32)
    grads_one = [None, None]
    grads_two = [None, None]
    for layer in (1, 0):
        h_in, pre_act, act_bf = saved[layer]
        resid_bf = resid_grad.astype(jnp.bfloat16)
        grads_two[layer] = jnp.dot(act_bf.T, resid_bf, preferred_element_type=jnp.float32)
        act_grad = jnp.dot(resid_bf, w_two[layer].T, preferred_element_type=jnp.float32)
        gelu_back = jax.vjp(jax.nn.gelu, pre_act)[1]
        pre_grad = gelu_back(act_grad)[0].astype(jnp.bfloat16)
        grads_one[layer] = jnp.dot(h_in.T, pre_grad, preferred_element_type=jnp.float32)
        if layer == 1:
            resid_grad = resid_grad + jnp.dot(pre_grad, w_one[layer].T, preferred_element_type=jnp.float32)
    return jnp.stack(grads_one), jnp.stack(grads_two), g_proj


def tower_grads(row_blocks, up_blocks, w_one, w_two, w_proj):
    def body(running, block_in):
        row_block, upstream = block_in
        hidden, saved = tower_forward(row_block, w_one, w_two, w_proj)[1:]
        new_grads = tower_backward(upstream, w_one, w_two, w_proj, hidden, saved)
        return tuple(old_sum + new_part for old_sum, new_part in zip(running, new_grads)), None

    zeros_init = (jnp.zeros(w_one.shape, jnp.float32), jnp.zeros(w_two.shape, jnp.float32), jnp.zeros(w_proj.shape, jnp.float32))
    return lax.scan(body, zeros_init, (row_blocks, up_blocks))[0]


def reference(q_in, d_in, temperature, q_w1, q_w2, q_proj, d_w1, d_w2, d_proj):
    n_blocks = GLOBAL_BATCH // SHARD_ROWS
    q_blocks = q_in.reshape(n_blocks, SHARD_ROWS, HIDDEN)
    d_blocks = d_in.reshape(n_blocks, 2 * SHARD_ROWS, HIDDEN)
    q_reps = lax.map(lambda row_block: tower_forward(row_block, q_w1, q_w2, q_proj)[0], q_blocks)
    doc_flat = lax.map(lambda row_block: tower_forward(row_block, d_w1, d_w2, d_proj)[0], d_blocks).reshape(2 * GLOBAL_BATCH, REPR_DIM)
    col_index = jnp.arange(2 * GLOBAL_BATCH)

    def loss_block(running, block_in):
        loss_sum, doc_grad = running
        q_block, block_index = block_in
        logits = jnp.dot(q_block, doc_flat.T, preferred_element_type=jnp.float32) / temperature
        row_index = block_index * SHARD_ROWS + jnp.arange(SHARD_ROWS)
        target = col_index[None, :] == row_index[:, None]
        log_norm = jax.nn.logsumexp(logits, axis=1)
        pos_logit = jnp.sum(jnp.where(target, logits, 0.0), axis=1)
        soft_prob = jnp.exp(logits - log_norm[:, None])
        grad_logit = ((soft_prob - target.astype(jnp.float32)) / (GLOBAL_BATCH * temperature)).astype(jnp.bfloat16)
        q_up = jnp.dot(grad_logit, doc_flat, preferred_element_type=jnp.float32).astype(jnp.bfloat16)
        doc_grad = doc_grad + jnp.dot(grad_logit.T, q_block, preferred_element_type=jnp.float32)
        return (loss_sum + jnp.sum(log_norm - pos_logit), doc_grad), q_up

    zeros_init = (jnp.zeros((), jnp.float32), jnp.zeros((2 * GLOBAL_BATCH, REPR_DIM), jnp.float32))
    final_state, q_up_blocks = lax.scan(loss_block, zeros_init, (q_reps, jnp.arange(n_blocks)))
    loss_sum, doc_grad = final_state
    doc_up_blocks = doc_grad.astype(jnp.bfloat16).reshape(n_blocks, 2 * SHARD_ROWS, REPR_DIM)
    q_one, q_two, q_pgrad = tower_grads(q_blocks, q_up_blocks, q_w1, q_w2, q_proj)
    d_one, d_two, d_pgrad = tower_grads(d_blocks, doc_up_blocks, d_w1, d_w2, d_proj)
    return (loss_sum / GLOBAL_BATCH, q_one, q_two, q_pgrad, d_one, d_two, d_pgrad)
```

```python
import functools

import jax
import jax.numpy as jnp
import numpy as np
from jax import lax
from jax.experimental import pallas as pl
from jax.experimental.pallas import tpu as pltpu
from jax.sharding import PartitionSpec as P

SUB_COUNT = 4
ND = 16
ROWS = 512
WIDTH = 384
FFN = 1536
BATCH = ROWS * ND
CHUNK = 2 * ROWS
BLOCKS = 17
HALF_ROWS = BLOCKS * WIDTH // 2
PART_ROWS = HALF_ROWS // 3
PIECE = PART_ROWS // 8
COLS = 512
MESH = pl.DeviceIdType.MESH
VMEM_MAX = 67_043_328
F32, BF16 = jnp.float32, jnp.bfloat16
K0 = float(np.sqrt(2.0 / np.pi).astype(np.float32))
LOW = -3.0e38
LOG2E = float(1.0 / np.log(2.0))

LAST = (((1,), (1,)), ((), ()))
FIRST = (((0,), (0,)), ((), ()))
NORMAL = (((1,), (0,)), ((), ()))


def mm(a, b, dims=NORMAL):
    return lax.dot_general(a, b, dims, preferred_element_type=F32)


def gelu(a):
    return a * (0.5 * (1.0 + jnp.tanh(K0 * (a + 0.044715 * (a * a * a)))))


def gelu_and_slope(a):
    sq = a * a
    t = jnp.tanh(K0 * (a + 0.044715 * (a * sq)))
    cdf = 0.5 * (1.0 + t)
    slope = cdf + a * (0.5 * (1.0 - t * t)) * (K0 + (3.0 * 0.044715 * K0) * sq)
    return a * cdf, slope


def forward_kernel(x_ref, w1_ref, w2_ref, p_ref, y_ref, u_ref):
    h = x_ref[...]
    for k in range(2):
        for c in range(FFN // COLS):
            cs = slice(c * COLS, (c + 1) * COLS)
            u_ref[:, cs] = gelu(mm(h, w1_ref[k, :, cs])).astype(BF16)
        h = (h.astype(F32) + mm(u_ref[...], w2_ref[k])).astype(BF16)
    y_ref[...] = mm(h, p_ref[...]).astype(BF16)


def tower_forward(rows, w1, w2, p):
    n = rows.shape[0]
    m = n // SUB_COUNT
    whole = lambda a: pl.BlockSpec(a.shape, lambda i: (0,) * a.ndim)
    return pl.pallas_call(
        forward_kernel,
        grid=(SUB_COUNT,),
        out_shape=jax.ShapeDtypeStruct((n, WIDTH), BF16),
        in_specs=[pl.BlockSpec((m, WIDTH), lambda i: (i, 0)), whole(w1), whole(w2), whole(p)],
        out_specs=pl.BlockSpec((m, WIDTH), lambda i: (i, 0)),
        scratch_shapes=[pltpu.VMEM((m, FFN), BF16)],
        compiler_params=pltpu.CompilerParams(vmem_limit_bytes=40 << 20),
        cost_estimate=pl.CostEstimate(flops=n * 5_000_000, bytes_accessed=n * 1536 + 5_000_000, transcendentals=0),
        name="tower_forward",
    )(rows, w1, w2, p)


def backward_kernel(x_ref, g_ref, w1_ref, w2_ref, p_ref, out_ref, u_ref, s_ref, h_ref, dl_ref):
    @pl.when(pl.program_id(0) == 0)
    def _():
        out_ref[...] = jnp.zeros_like(out_ref)

    h_ref[0] = x_ref[...]
    for k in range(2):
        h = h_ref[k]
        for c in range(FFN // COLS):
            cs = slice(c * COLS, (c + 1) * COLS)
            act, slope = gelu_and_slope(mm(h, w1_ref[k, :, cs]))
            u_ref[k, :, cs] = act.astype(BF16)
            s_ref[k, :, cs] = slope
        h_ref[k + 1] = (h.astype(F32) + mm(u_ref[k], w2_ref[k])).astype(BF16)
    g = g_ref[...]
    out_ref[16] += mm(h_ref[2], g, FIRST)
    e = mm(g, p_ref[...], LAST)
    for k in (1, 0):
        eb = e.astype(BF16)
        for c in range(4):
            out_ref[8 + 4 * k + c] += mm(u_ref[k, :, c * WIDTH:(c + 1) * WIDTH], eb, FIRST)
        for c in range(FFN // COLS):
            cs = slice(c * COLS, (c + 1) * COLS)
            dl_ref[:, cs] = (s_ref[k, :, cs] * mm(eb, w2_ref[k, cs, :], LAST)).astype(BF16)
        for c in range(2):
            part = mm(h_ref[k], dl_ref[:, 2 * c * WIDTH:2 * (c + 1) * WIDTH], FIRST)
            out_ref[4 * k + 2 * c] += part[:, :WIDTH]
            out_ref[4 * k + 2 * c + 1] += part[:, WIDTH:]
        if k == 1:
            e = e + mm(dl_ref[...], w1_ref[k], LAST)


def tower_backward(rows, up, w1, w2, p):
    n = rows.shape[0]
    m = n // SUB_COUNT
    whole = lambda a: pl.BlockSpec(a.shape, lambda i: (0,) * a.ndim)
    block = pl.BlockSpec((m, WIDTH), lambda i: (i, 0))
    return pl.pallas_call(
        backward_kernel,
        grid=(SUB_COUNT,),
        out_shape=jax.ShapeDtypeStruct((BLOCKS, WIDTH, WIDTH), F32),
        in_specs=[block, block, whole(w1), whole(w2), whole(p)],
        out_specs=pl.BlockSpec((BLOCKS, WIDTH, WIDTH), lambda i: (0, 0, 0)),
        scratch_shapes=[
            pltpu.VMEM((2, m, FFN), BF16),
            pltpu.VMEM((2, m, FFN), F32),
            pltpu.VMEM((3, m, WIDTH), BF16),
            pltpu.VMEM((m, FFN), BF16),
        ],
        compiler_params=pltpu.CompilerParams(vmem_limit_bytes=60 << 20),
        cost_estimate=pl.CostEstimate(flops=n * 15_000_000, bytes_accessed=n * 1536 + 15_000_000, transcendentals=0),
        name="tower_backward",
    )(rows, up, w1, w2, p)


def unpack(blocks):
    w1 = blocks[:8].reshape(2, 4, WIDTH, WIDTH).transpose(0, 2, 1, 3).reshape(2, WIDTH, FFN)
    return w1, blocks[8:16].reshape(2, FFN, WIDTH), blocks[16]


def bit_of(me, b):
    return lax.rem(me // (1 << b), 2)


def across(me, b):
    return me + (1 - 2 * bit_of(me, b)) * (1 << b)


def piece_rows(me, core, part, r):
    at = 0
    for i in range(3):
        bit = bit_of(me, 1 + (part + i) % 3)
        at = 2 * at + ((1 - bit) if (r >> (2 - i)) & 1 else bit)
    return pl.ds(pl.multiple_of(core * HALF_ROWS + part * PART_ROWS + at * PIECE, 8), PIECE)


def sum_kernel(x_ref, out_ref, acc, r0, r1, r2, r3, s0, s1, s2, s3, v0, v1, v2, v3, t0, t1, t2, t3, w0, w1, w2, w3):
    me = lax.axis_index("data")
    core = bit_of(me, 0)
    barrier = pltpu.get_barrier_semaphore()
    for b in range(4):
        pl.semaphore_signal(barrier, inc=1, device_id=(across(me, b),), device_id_type=MESH)
    pl.semaphore_wait(barrier, 4)

    def send(src, dst, send_sem, recv_sem, b):
        return pltpu.make_async_remote_copy(
            src_ref=src, dst_ref=dst, send_sem=send_sem, recv_sem=recv_sem,
            device_id=(across(me, b),), device_id_type=MESH)

    def mine(part, r):
        return piece_rows(me, core, part, r)

    def dim(part, i):
        return 1 + (part + i) % 3

    def swap(part, r):
        return send(x_ref.at[piece_rows(me, 1 - core, part, r)], r0.at[8 * part + r], s0.at[8 * part + r], v0.at[8 * part + r], 0)

    def first(part, r):
        return send(acc.at[8 * part + 4 + r], r1.at[4 * part + r], s1.at[4 * part + r], v1.at[4 * part + r], dim(part, 0))

    def second(part, r):
        return send(acc.at[8 * part + 2 + r], r2.at[2 * part + r], s2.at[2 * part + r], v2.at[2 * part + r], dim(part, 1))

    def third(part):
        return send(acc.at[8 * part + 1], r3.at[part], s3.at[part], v3.at[part], dim(part, 2))

    def back(part, r, level, theirs=False):
        if level == 3:
            where = piece_rows(me, 1 - core, part, r) if theirs else mine(part, r)
            k = 8 * part + r
            return send(out_ref.at[where], out_ref.at[where], t0.at[k], w0.at[k], 0)
        (ss, rs), n = (((t1, w1), 4), ((t2, w2), 2), ((t3, w3), 1))[level]
        where = mine(part, r + n) if theirs else mine(part, r)
        return send(out_ref.at[where], out_ref.at[where], ss.at[n * part + r], rs.at[n * part + r], dim(part, level))

    order = (7, 6, 5, 4, 3, 2, 1, 0)
    parts = range(3)
    for r in order:
        for p in parts:
            swap(p, r).start()
    for r in order:
        for p in parts:
            swap(p, r).wait_recv()
            acc[8 * p + r] = x_ref[mine(p, r), :] + r0[8 * p + r]
            if r >= 4:
                first(p, r - 4).start()
    for r in (3, 2):
        for p in parts:
            first(p, r).wait_recv()
            acc[8 * p + r] = acc[8 * p + r] + r1[4 * p + r]
            second(p, r - 2).start()
    for p in parts:
        first(p, 1).wait_recv()
        second(p, 1).wait_recv()
        acc[8 * p + 1] = acc[8 * p + 1] + r1[4 * p + 1] + r2[2 * p + 1]
        third(p).start()
    for p in parts:
        first(p, 0).wait_recv()
        second(p, 0).wait_recv()
        acc[8 * p] = acc[8 * p] + r1[4 * p] + r2[2 * p]
    for p in parts:
        third(p).wait_recv()
        out_ref[mine(p, 0), :] = acc[8 * p] + r3[p]
        back(p, 0, 2).start()
    for level in (1, 0, 3):
        for p in parts:
            back(p, 0, level).start()
    for p in parts:
        back(p, 0, 2, True).wait_recv()
        back(p, 1, 1).start()
    for p in parts:
        back(p, 1, 0).start()
        back(p, 1, 3).start()
    for r in (0, 1):
        for p in parts:
            back(p, r, 1, True).wait_recv()
            back(p, 2 + r, 0).start()
            back(p, 2 + r, 3).start()
    for r in range(4):
        for p in parts:
            back(p, r, 0, True).wait_recv()
            back(p, 4 + r, 3).start()
    for r in range(8):
        for p in parts:
            back(p, r, 3, True).wait_recv()
    for p in parts:
        for r in range(8):
            swap(p, r).wait_send()
            back(p, r, 3).wait_send()
        for r in range(4):
            first(p, r).wait_send()
            back(p, r, 0).wait_send()
        for r in range(2):
            second(p, r).wait_send()
            back(p, r, 1).wait_send()
        third(p).wait_send()
        back(p, 0, 2).wait_send()


def sum_devices(blocks):
    x = blocks.reshape(BLOCKS * WIDTH, WIDTH)
    vmem = pl.BlockSpec(memory_space=pltpu.VMEM)
    counts = (24, 12, 6, 3)
    out = pl.pallas_call(
        sum_kernel,
        out_shape=jax.ShapeDtypeStruct(x.shape, F32),
        in_specs=[vmem],
        out_specs=vmem,
        scratch_shapes=[pltpu.VMEM((24, PIECE, WIDTH), F32)]
        + [pltpu.VMEM((n, PIECE, WIDTH), F32) for n in counts]
        + [pltpu.SemaphoreType.DMA((n,)) for n in counts * 4],
        compiler_params=pltpu.CompilerParams(collective_id=1, has_side_effects=True, vmem_limit_bytes=60 << 20),
        name="sum_devices",
    )(x)
    return out.reshape(blocks.shape)


def gather_kernel(tau_ref, docs_own, x_ref, w1_ref, w2_ref, p_ref, up_ref, stat_ref, q_all, docs, e_ref, m_ref, g_ref, acc, u_ref,
                  q_ref, mine_ref, *sems):
    me = lax.axis_index("data")
    d_sems, q_sems, (share_send, share_recv, local_sem) = sems[:8], sems[8:16], sems[16:]
    inv_tau = 1.0 / tau_ref[0]
    c = inv_tau * LOG2E
    scale = inv_tau / BATCH
    parts = range(3)

    barrier = pltpu.get_barrier_semaphore()
    for p in range(1, ND):
        pl.semaphore_signal(barrier, inc=1, device_id=(lax.rem(me + p, ND),), device_id_type=MESH)
    pl.semaphore_wait(barrier, ND - 1)

    def place(part, r, other=0):
        dev = across(me, 0) if other else me
        for i in range(3):
            if (r >> (2 - i)) & 1:
                dev = dev + (1 - 2 * bit_of(me, 1 + (part + i) % 3)) * (1 << (1 + (part + i) % 3))
        return dev

    def hop(own, everyone, cuts, sem, part, r, level, theirs=False):
        n = (4, 2, 1, 8)[level]
        ss, rs = sem[2 * level], sem[2 * level + 1]
        rows, lo, hi = own.shape[0], cuts[part], cuts[part + 1]

        def at(dev):
            return pl.ds(pl.multiple_of(dev * rows + lo, 16), hi - lo)

        if theirs:
            src = dst = everyone.at[at(place(part, r, 1) if level == 3 else place(part, r + n))]
        else:
            dst = everyone.at[at(place(part, r))]
            src = own.at[pl.ds(lo, hi - lo)] if r == 0 else dst
        return pltpu.make_async_remote_copy(
            src_ref=src, dst_ref=dst, send_sem=ss.at[n * part + r], recv_sem=rs.at[n * part + r],
            device_id=(across(me, 0 if level == 3 else 1 + (part + level) % 3),), device_id_type=MESH)

    doc = functools.partial(hop, docs_own, docs, (0, 336, 672, 1024), d_sems)
    qry = functools.partial(hop, q_ref, q_all, (0, 176, 352, 512), q_sems)

    def begin(f):
        for level in (2, 1, 0, 3):
            for p in parts:
                f(p, 0, level).start()

    def tick_one(f):
        for p in parts:
            f(p, 0, 2, True).wait_recv()
            f(p, 1, 1).start()
        for p in parts:
            f(p, 1, 0).start()
            f(p, 1, 3).start()

    def tick_two(f, r):
        for p in parts:
            f(p, r, 1, True).wait_recv()
            f(p, 2 + r, 0).start()
            f(p, 2 + r, 3).start()

    def tick_last(f, rs):
        for r in rs:
            for p in parts:
                f(p, r, 0, True).wait_recv()
                f(p, 4 + r, 3).start()

    def tick_core(f, rs):
        for r in rs:
            for p in parts:
                f(p, r, 3, True).wait_recv()

    def drain(f):
        for p in parts:
            for level, n in ((0, 4), (1, 2), (2, 1), (3, 8)):
                for r in range(n):
                    f(p, r, level).wait_send()

    begin(doc)
    docs[pl.ds(pl.multiple_of(me * CHUNK, CHUNK), CHUNK), :] = docs_own[...]
    m = ROWS // SUB_COUNT

    def forward(i, _):
        at = pl.ds(pl.multiple_of(i * m, m), m)
        h = x_ref[at, :]
        for k in range(2):
            for j in range(FFN // COLS):
                cs = slice(j * COLS, (j + 1) * COLS)
                u_ref[:, cs] = gelu(mm(h, w1_ref[k, :, cs])).astype(BF16)
            h = (h.astype(F32) + mm(u_ref[...], w2_ref[k])).astype(BF16)
        q_ref[at, :] = mm(h, p_ref[...]).astype(BF16)
        return 0

    lax.fori_loop(0, SUB_COUNT, forward, 0)
    local = pltpu.make_async_copy(q_ref, q_all.at[pl.ds(pl.multiple_of(me * ROWS, ROWS), ROWS)], local_sem)
    local.start()
    tick_one(doc)
    m_ref[...] = jnp.full_like(m_ref, LOW)
    lane = lax.broadcasted_iota(jnp.int32, (ROWS, 128), 1)

    def device_at(k):
        chip = k // 2
        chip = jnp.where(chip == 3, 4, jnp.where(chip == 4, 3, chip))
        flips = 2 * chip + lax.rem(k, 2)
        return me + sum((1 - 2 * bit_of(me, b)) * (1 << b) * lax.rem(flips // (1 << b), 2) for b in range(4))

    def score(k, carry):
        @pl.when(k == 1)
        def _():
            tick_core(doc, (0,))

        @pl.when(k == 2)
        def _():
            tick_two(doc, 0)
            tick_last(doc, (0,))

        @pl.when(k == 3)
        def _():
            tick_core(doc, (1, 2, 4))

        @pl.when(k == 8)
        def _():
            tick_two(doc, 1)
            begin(qry)
            tick_last(doc, (1, 2))

        @pl.when(k == 9)
        def _():
            tick_core(doc, (3, 5, 6))

        @pl.when(k == 14)
        def _():
            tick_last(doc, (3,))

        @pl.when(k == 15)
        def _():
            tick_core(doc, (7,))

        top, total = carry
        base = device_at(k) * CHUNK
        marks = m_ref[...]
        for half in range(2):
            rows = docs[pl.ds(pl.multiple_of(base + half * ROWS, ROWS), ROWS), :]
            s = mm(q_ref[...], rows, LAST)
            best = jnp.max(s, axis=1, keepdims=True)
            e = jnp.exp2((s - best) * c)
            e_ref[k, :, half * ROWS:(half + 1) * ROWS] = e
            marks = jnp.where(lane == 2 * k + half, best, marks)
            new_top = jnp.maximum(top, best)
            total = total * jnp.exp2((top - new_top) * c) + jnp.sum(e, axis=1, keepdims=True) * jnp.exp2((best - new_top) * c)
            top = new_top
        m_ref[...] = marks
        return top, total

    top, total = lax.fori_loop(0, ND, score, (jnp.full((ROWS, 1), LOW, F32), jnp.zeros((ROWS, 1), F32)))
    pos = jnp.sum(q_ref[...].astype(F32) * docs_own[0:ROWS, :].astype(F32), axis=1, keepdims=True)
    loss = (top - pos) * inv_tau + jnp.log(total)
    weight = scale / total
    mine_ref[...] = jnp.where(lane == 0, top, jnp.where(lane == 1, weight, loss)).T[0:8, :]
    stat_ref[me] = mine_ref[...]

    def share(p, slot):
        return pltpu.make_async_remote_copy(
            src_ref=mine_ref, dst_ref=stat_ref.at[slot], send_sem=share_send.at[p], recv_sem=share_recv.at[p],
            device_id=(lax.rem(me + p, ND),), device_id_type=MESH)

    for p in range(1, ND):
        share(p, me).start()
    m_ref[...] = jnp.exp2((m_ref[...] - top) * c) * weight
    tick_one(qry)

    def weighted(k, half):
        f = jnp.sum(jnp.where(lane == 2 * k + half, m_ref[...], 0.0), axis=1, keepdims=True)
        return e_ref[k, :, half * ROWS:(half + 1) * ROWS] * f

    r = lax.broadcasted_iota(jnp.int32, (ROWS, ROWS), 0)
    col = lax.broadcasted_iota(jnp.int32, (ROWS, ROWS), 1)
    acc[...] = mm((weighted(0, 0) - jnp.where(r == col, scale, 0.0)).astype(BF16), docs_own[0:ROWS, :])
    acc[...] += mm(weighted(0, 1).astype(BF16), docs_own[ROWS:, :])

    def pull(k, _):
        @pl.when(k == 5)
        def _():
            tick_two(qry, 0)
            tick_last(qry, (0,))

        @pl.when(k == 10)
        def _():
            tick_two(qry, 1)

        base = device_at(k) * CHUNK
        for half in range(2):
            g_ref[:, half * ROWS:(half + 1) * ROWS] = weighted(k, half).astype(BF16)
        acc[...] += mm(g_ref[...], docs[pl.ds(pl.multiple_of(base, CHUNK), CHUNK), :])
        return 0

    lax.fori_loop(1, ND, pull, 0)
    up_ref[...] = acc[...].astype(BF16)
    tick_last(qry, (1, 2, 3))
    tick_core(qry, range(8))
    for p in range(1, ND):
        share(p, me).wait_send()
        share(p, lax.rem(me + ND - p, ND)).wait_recv()
    drain(doc)
    drain(qry)
    local.wait()


def gather_rows(tau, docs_own, x, w1, w2, p):
    vmem = pl.BlockSpec(memory_space=pltpu.VMEM)
    hops = [pltpu.SemaphoreType.DMA((3 * n,)) for n in (4, 4, 2, 2, 1, 1, 8, 8)]
    return pl.pallas_call(
        gather_kernel,
        out_shape=[
            jax.ShapeDtypeStruct((ROWS, WIDTH), BF16),
            jax.ShapeDtypeStruct((ND, 8, ROWS), F32),
            jax.ShapeDtypeStruct((BATCH, WIDTH), BF16),
        ],
        in_specs=[pl.BlockSpec(memory_space=pltpu.SMEM)] + [vmem] * 5,
        out_specs=[vmem, vmem, pl.BlockSpec(memory_space=pl.ANY)],
        scratch_shapes=[
            pltpu.VMEM((2 * BATCH, WIDTH), BF16),
            pltpu.VMEM((ND, ROWS, CHUNK), F32),
            pltpu.VMEM((ROWS, 128), F32),
            pltpu.VMEM((ROWS, CHUNK), BF16),
            pltpu.VMEM((ROWS, WIDTH), F32),
            pltpu.VMEM((ROWS // SUB_COUNT, FFN), BF16),
            pltpu.VMEM((ROWS, WIDTH), BF16),
            pltpu.VMEM((8, ROWS), F32),
        ] + hops + hops + [pltpu.SemaphoreType.DMA((ND,)), pltpu.SemaphoreType.DMA((ND,)), pltpu.SemaphoreType.DMA],
        compiler_params=pltpu.CompilerParams(collective_id=0, has_side_effects=True, vmem_limit_bytes=VMEM_MAX),
        cost_estimate=pl.CostEstimate(flops=15_000_000_000, bytes_accessed=14_000_000, transcendentals=0),
        name="gather_rows",
    )(tau, docs_own, x, w1, w2, p)


def col_kernel(tau_ref, stat_ref, own_ref, q_ref, up_ref, q_all, g_ref, acc, sems):
    me = lax.axis_index("data")
    inv_tau = 1.0 / tau_ref[0]
    c = inv_tau * LOG2E
    scale = inv_tau / BATCH

    def rows_of(k):
        return pl.ds(pl.multiple_of(lax.rem(me + k, ND) * ROWS, ROWS), ROWS)

    def chunk_copy(k):
        return pltpu.make_async_copy(q_ref.at[rows_of(k)], q_all.at[rows_of(k)], sems.at[k])

    for k in range(ND):
        chunk_copy(k).start()

    def probs(k):
        j = lax.rem(me + k, ND)
        s = mm(own_ref[...], q_all[rows_of(k), :], LAST)
        return jnp.exp2((s - stat_ref[j, 0:1, :]) * c) * stat_ref[j, 1:2, :]

    chunk_copy(0).wait()
    prob = probs(0)
    r = lax.broadcasted_iota(jnp.int32, (CHUNK, ROWS), 0)
    col = lax.broadcasted_iota(jnp.int32, (CHUNK, ROWS), 1)
    acc[...] = mm((prob - jnp.where(r == col, scale, 0.0)).astype(BF16), q_all[rows_of(0), :])

    def step(i, _):
        for n in range(3):
            k = 3 * i + n + 1
            chunk_copy(k).wait()
            g_ref[n] = probs(k).astype(BF16)
            acc[...] += mm(g_ref[n], q_all[rows_of(k), :])
        return 0

    lax.fori_loop(0, 5, step, 0)
    up_ref[...] = acc[...].astype(BF16)


def loss_cols(tau, stats, own, q_all):
    vmem = pl.BlockSpec(memory_space=pltpu.VMEM)
    return pl.pallas_call(
        col_kernel,
        out_shape=jax.ShapeDtypeStruct((CHUNK, WIDTH), BF16),
        in_specs=[pl.BlockSpec(memory_space=pltpu.SMEM), vmem, vmem, pl.BlockSpec(memory_space=pl.ANY)],
        out_specs=vmem,
        scratch_shapes=[
            pltpu.VMEM((BATCH, WIDTH), BF16),
            pltpu.VMEM((3, CHUNK, ROWS), BF16),
            pltpu.VMEM((CHUNK, WIDTH), F32),
            pltpu.SemaphoreType.DMA((ND,)),
        ],
        compiler_params=pltpu.CompilerParams(vmem_limit_bytes=60 << 20),
        cost_estimate=pl.CostEstimate(flops=13_000_000_000, bytes_accessed=8_000_000, transcendentals=0),
        name="loss_cols",
    )(tau, stats, own, q_all)


def local_step(q_loc, d_loc, temperature, q_w1, q_w2, q_proj, d_w1, d_w2, d_proj):
    tau = temperature.reshape(1)
    d_rows = d_loc.reshape(CHUNK, WIDTH)
    d_reps = tower_forward(d_rows, d_w1, d_w2, d_proj)
    q_up, stats, q_all = gather_rows(tau, d_reps, q_loc, q_w1, q_w2, q_proj)
    loss = jnp.sum(stats[:, 2, :]) / BATCH
    q_grads = tower_backward(q_loc, q_up, q_w1, q_w2, q_proj)
    q_sum = lax.psum(q_grads, "data")
    stats, q_grads = lax.optimization_barrier((stats, q_grads))
    d_up = loss_cols(tau, stats, d_reps, q_all)
    d_sum = sum_devices(tower_backward(d_rows, d_up, d_w1, d_w2, d_proj))
    return (loss, *unpack(q_sum), *unpack(d_sum))


def solution(mesh):
    specs_in = (P("data", None), P(None, "data", None), P(), P(), P(), P(), P(), P(), P())
    specs_out = (P(), P(), P(), P(), P(), P(), P())
    return jax.shard_map(local_step, mesh=mesh, in_specs=specs_in, out_specs=specs_out, check_vma=False)
```

```python
import functools

import jax
import jax.numpy as jnp
import numpy as np
from jax import lax
from jax.experimental import pallas as pl
from jax.experimental.pallas import tpu as pltpu
from jax.sharding import PartitionSpec as P

SUB_COUNT = 4
ND = 16
ROWS = 512
WIDTH = 384
FFN = 1536
BATCH = ROWS * ND
CHUNK = 2 * ROWS
BLOCKS = 17
HALF_ROWS = BLOCKS * WIDTH // 2
PART_ROWS = HALF_ROWS // 3
PIECE = PART_ROWS // 8
PARTS = range(3)
NEAR, FAR = range(3, -1, -1), range(7, 3, -1)
HOPS = (4, 2, 1, 8)
COLS = 512
TILES = range(FFN // COLS)
MESH = pl.DeviceIdType.MESH
VMEM_MAX = 67_043_328
F32, BF16 = jnp.float32, jnp.bfloat16
K0 = float(np.sqrt(2.0 / np.pi).astype(np.float32))
LOW = -3.0e38
LOG2E = float(1.0 / np.log(2.0))

LAST = (((1,), (1,)), ((), ()))
FIRST = (((0,), (0,)), ((), ()))
NORMAL = (((1,), (0,)), ((), ()))


def mm(a, b, dims=NORMAL):
    return lax.dot_general(a, b, dims, preferred_element_type=F32)


def gelu(a):
    return a * (0.5 * (1.0 + jnp.tanh(K0 * (a + 0.044715 * (a * a * a)))))


def gelu_and_slope(a):
    sq = a * a
    t = jnp.tanh(K0 * (a + 0.044715 * (a * sq)))
    cdf = 0.5 * (1.0 + t)
    slope = cdf + a * (0.5 * (1.0 - t * t)) * (K0 + (3.0 * 0.044715 * K0) * sq)
    return a * cdf, slope


def forward_kernel(x_ref, w1_ref, w2_ref, p_ref, y_ref, u_ref):
    h = x_ref[...]
    for k in range(2):
        for c in TILES:
            cs = slice(c * COLS, (c + 1) * COLS)
            u_ref[:, cs] = gelu(mm(h, w1_ref[k, :, cs])).astype(BF16)
        h = (h.astype(F32) + mm(u_ref[...], w2_ref[k])).astype(BF16)
    y_ref[...] = mm(h, p_ref[...]).astype(BF16)


def tower_forward(rows, w1, w2, p):
    n = rows.shape[0]
    m = n // SUB_COUNT
    whole = lambda a: pl.BlockSpec(a.shape, lambda i: (0,) * a.ndim)
    return pl.pallas_call(
        forward_kernel,
        grid=(SUB_COUNT,),
        out_shape=jax.ShapeDtypeStruct((n, WIDTH), BF16),
        in_specs=[pl.BlockSpec((m, WIDTH), lambda i: (i, 0)), whole(w1), whole(w2), whole(p)],
        out_specs=pl.BlockSpec((m, WIDTH), lambda i: (i, 0)),
        scratch_shapes=[pltpu.VMEM((m, FFN), BF16)],
        compiler_params=pltpu.CompilerParams(vmem_limit_bytes=40 << 20),
        name="tower_forward",
    )(rows, w1, w2, p)


def backward_rows(x, g, w1_ref, w2_ref, p_ref, add, u_ref, s_ref, h_ref, dl_ref, middle=None):
    h_ref[0] = x
    for k in range(2):
        h = h_ref[k]
        for c in TILES:
            cs = slice(c * COLS, (c + 1) * COLS)
            act, slope = gelu_and_slope(mm(h, w1_ref[k, :, cs]))
            u_ref[k, :, cs] = act.astype(BF16)
            s_ref[k, :, cs] = slope
        h_ref[k + 1] = (h.astype(F32) + mm(u_ref[k], w2_ref[k])).astype(BF16)
    if middle is not None:
        middle()
    add(16, mm(h_ref[2], g, FIRST))
    e = mm(g, p_ref[...], LAST)
    for k in (1, 0):
        eb = e.astype(BF16)
        for c in range(4):
            add(8 + 4 * k + c, mm(u_ref[k, :, c * WIDTH:(c + 1) * WIDTH], eb, FIRST))
        for c in TILES:
            cs = slice(c * COLS, (c + 1) * COLS)
            dl_ref[:, cs] = (s_ref[k, :, cs] * mm(eb, w2_ref[k, cs, :], LAST)).astype(BF16)
        for c in range(2):
            part = mm(h_ref[k], dl_ref[:, 2 * c * WIDTH:2 * (c + 1) * WIDTH], FIRST)
            add(4 * k + 2 * c, part[:, :WIDTH])
            add(4 * k + 2 * c + 1, part[:, WIDTH:])
        if k == 1:
            e = e + mm(dl_ref[...], w1_ref[k], LAST)


def backward_kernel(x_ref, g_ref, w1_ref, w2_ref, p_ref, out_ref, u_ref, s_ref, h_ref, dl_ref):
    @pl.when(pl.program_id(0) == 0)
    def _():
        out_ref[...] = jnp.zeros_like(out_ref)

    def add(block, value):
        out_ref[block] += value

    backward_rows(x_ref[...], g_ref[...], w1_ref, w2_ref, p_ref, add, u_ref, s_ref, h_ref, dl_ref)


def tower_backward(rows, up, w1, w2, p):
    n = rows.shape[0]
    m = n // SUB_COUNT
    whole = lambda a: pl.BlockSpec(a.shape, lambda i: (0,) * a.ndim)
    block = pl.BlockSpec((m, WIDTH), lambda i: (i, 0))
    return pl.pallas_call(
        backward_kernel,
        grid=(SUB_COUNT,),
        out_shape=jax.ShapeDtypeStruct((BLOCKS, WIDTH, WIDTH), F32),
        in_specs=[block, block, whole(w1), whole(w2), whole(p)],
        out_specs=pl.BlockSpec((BLOCKS, WIDTH, WIDTH), lambda i: (0, 0, 0)),
        scratch_shapes=[
            pltpu.VMEM((2, m, FFN), BF16),
            pltpu.VMEM((2, m, FFN), F32),
            pltpu.VMEM((3, m, WIDTH), BF16),
            pltpu.VMEM((m, FFN), BF16),
        ],
        compiler_params=pltpu.CompilerParams(vmem_limit_bytes=60 << 20),
        name="tower_backward",
    )(rows, up, w1, w2, p)


def unpack_kernel(q_ref, d_ref, *refs):
    outs, hold, load, store = refs[:6], refs[6], refs[7], refs[8]

    def place(j):
        w1, w2, p = outs[3 * (j // BLOCKS):3 * (j // BLOCKS) + 3]
        n = j % BLOCKS
        if n < 8:
            return w1.at[n // 4, :, pl.ds(n % 4 * WIDTH, WIDTH)]
        if n < 16:
            return w2.at[(n - 8) // 4, pl.ds(n % 4 * WIDTH, WIDTH), :]
        return p

    def fetch(j):
        return pltpu.make_async_copy((q_ref, d_ref)[j // BLOCKS].at[j % BLOCKS], hold.at[j], load.at[j])

    def put(j):
        return pltpu.make_async_copy(hold.at[j], place(j), store.at[j])

    for j in range(2 * BLOCKS):
        fetch(j).start()
    for j in range(2 * BLOCKS):
        fetch(j).wait()
        put(j).start()
    for j in range(2 * BLOCKS):
        put(j).wait()


def unpack(q_blocks, d_blocks, shapes):
    hbm = pl.BlockSpec(memory_space=pl.ANY)
    return pl.pallas_call(
        unpack_kernel,
        out_shape=[jax.ShapeDtypeStruct(a, F32) for a in shapes],
        in_specs=[hbm, hbm],
        out_specs=[hbm] * 6,
        scratch_shapes=[
            pltpu.VMEM((2 * BLOCKS, WIDTH, WIDTH), F32),
            pltpu.SemaphoreType.DMA((2 * BLOCKS,)),
            pltpu.SemaphoreType.DMA((2 * BLOCKS,)),
        ],
        compiler_params=pltpu.CompilerParams(vmem_limit_bytes=24 << 20),
        name="unpack",
    )(q_blocks, d_blocks)


def bit_of(me, b):
    return lax.rem(me // (1 << b), 2)


def across(me, b):
    return me + (1 - 2 * bit_of(me, b)) * (1 << b)


def sum_places(me):
    core, bits = bit_of(me, 0), [bit_of(me, b) for b in (1, 2, 3)]
    mine, partner = [], []
    for p in PARTS:
        side = [(bits[(p + i) % 3] * (4 >> i) * PIECE, (1 - bits[(p + i) % 3]) * (4 >> i) * PIECE) for i in range(3)]
        for r in range(8):
            at = p * PART_ROWS + side[0][r >> 2] + side[1][(r >> 1) & 1] + side[2][r & 1]
            mine.append(pl.ds(pl.multiple_of(core * HALF_ROWS + at, 8), PIECE))
            partner.append(pl.ds(pl.multiple_of((1 - core) * HALF_ROWS + at, 8), PIECE))
    return mine, partner, [across(me, b) for b in range(4)]


class Gather:
    def __init__(self, copy):
        self.copy = copy

    def begin(self):
        for level in (2, 1, 0, 3):
            for p in PARTS:
                self.copy(p, 0, level).start()

    def pass_on(self, level, *rs):
        for r in rs:
            for p in PARTS:
                self.copy(p, r, level, True).wait_recv()
                for lower in (*range(level - 1, -1, -1), 3):
                    self.copy(p, r + HOPS[level], lower).start()

    def core(self, *rs):
        for r in rs:
            for p in PARTS:
                self.copy(p, r, 3, True).wait_recv()

    def drain(self):
        for level, n in enumerate(HOPS):
            for r in range(n):
                for p in PARTS:
                    self.copy(p, r, level).wait_send()


HOP_SEMS = [pltpu.SemaphoreType.DMA((3 * n,)) for n in HOPS for _ in range(2)]


class DeviceSum:
    def __init__(self, places, own, other, out, bufs, sems, load=None):
        self.mine, self.partner, self.peers = places
        self.own, self.other, self.out, self.load = own, other, out, load
        self.bufs, self.sems = bufs, sems
        self.gather = Gather(self.back)

    def copy(self, src, dst, level, k, b):
        return pltpu.make_async_remote_copy(
            src_ref=src, dst_ref=dst, send_sem=self.sems[2 * level].at[k], recv_sem=self.sems[2 * level + 1].at[k],
            device_id=(self.peers[b],), device_id_type=MESH)

    def swap(self, p, r):
        return self.copy(self.other(p, r), self.bufs[0].at[8 * p + r], 0, 8 * p + r, 0)

    def link(self, p, r, level):
        n = HOPS[level]
        return self.copy(self.own(p, n + r), self.bufs[1 + level].at[n * p + r], 1 + level, n * p + r, 1 + (p + level) % 3)

    def back(self, p, r, level, theirs=False):
        n = HOPS[level]
        if theirs and level == 3:
            dst = self.out.at[self.partner[8 * p + r]]
        else:
            dst = self.out.at[self.mine[8 * p + (r + n if theirs else r)]]
        src = self.own(p, 0) if r == 0 and not theirs else dst
        return self.copy(src, dst, 4 + level, n * p + r, 0 if level == 3 else 1 + (p + level) % 3)

    def keep(self, p):
        return pltpu.make_async_copy(self.own(p, 0), self.out.at[self.mine[8 * p]], self.sems[16].at[p])

    def plus(self, p, r, *terms):
        ref = self.own(p, r)
        value = ref[...]
        for level, k in terms:
            value = value + self.bufs[level][k]
        ref[...] = value

    def start(self):
        for r in reversed(range(8)):
            for p in PARTS:
                if self.load is not None:
                    self.load(p, r).start()
                self.swap(p, r).start()

    def swapped(self, rs):
        for r in rs:
            for p in PARTS:
                if self.load is not None:
                    self.load(p, r).wait()
                self.swap(p, r).wait_recv()
                self.plus(p, r, (0, 8 * p + r))
                if r >= 4:
                    self.link(p, r - 4, 0).start()

    def second(self, r):
        for p in PARTS:
            self.link(p, r, 0).wait_recv()
            self.plus(p, r, (1, 4 * p + r))
            self.link(p, r - 2, 1).start()

    def third(self):
        for p in PARTS:
            self.link(p, 1, 0).wait_recv()
            self.link(p, 1, 1).wait_recv()
            self.plus(p, 1, (1, 4 * p + 1), (2, 2 * p + 1))
            self.link(p, 0, 2).start()

    def finish(self):
        for p in PARTS:
            self.link(p, 0, 0).wait_recv()
            self.link(p, 0, 1).wait_recv()
            self.link(p, 0, 2).wait_recv()
            self.plus(p, 0, (1, 4 * p), (2, 2 * p), (3, p))
        self.gather.begin()
        for p in PARTS:
            self.keep(p).start()

    def close(self):
        self.gather.core(*range(8))
        self.gather.drain()
        for p in PARTS:
            for r in range(8):
                self.swap(p, r).wait_send()
            for level in PARTS:
                for r in range(HOPS[level]):
                    self.link(p, r, level).wait_send()
            self.keep(p).wait()


SUM_BUFS = [pltpu.VMEM((n, PIECE, WIDTH), F32) for n in (24, 12, 6, 3)]
SUM_SEMS = [pltpu.SemaphoreType.DMA((n,)) for n in (24, 12, 6, 3) for _ in range(2)] + HOP_SEMS + [pltpu.SemaphoreType.DMA((3,))]


def gather_kernel(tau_ref, docs_own, x_ref, w1_ref, w2_ref, p_ref, up_ref, stat_ref, q_all, docs, e_ref, m_ref, g_ref, acc, u_ref,
                  q_ref, mine_ref, *sems):
    me = lax.axis_index("data")
    d_sems, q_sems, (share_send, share_recv, local_sem) = sems[:8], sems[8:16], sems[16:]
    inv_tau = 1.0 / tau_ref[0]
    c = inv_tau * LOG2E
    scale = inv_tau / BATCH
    barrier = pltpu.get_barrier_semaphore()
    for p in range(1, ND):
        pl.semaphore_signal(barrier, inc=1, device_id=(lax.rem(me + p, ND),), device_id_type=MESH)
    pl.semaphore_wait(barrier, ND - 1)

    def place(part, r, other=0):
        dev = across(me, 0) if other else me
        for i in range(3):
            if (r >> (2 - i)) & 1:
                dev = dev + (1 - 2 * bit_of(me, 1 + (part + i) % 3)) * (1 << (1 + (part + i) % 3))
        return dev

    def hop(own, everyone, cuts, sem, part, r, level, theirs=False):
        n = HOPS[level]
        ss, rs = sem[2 * level], sem[2 * level + 1]
        rows, lo, hi = own.shape[0], cuts[part], cuts[part + 1]

        def at(dev):
            return pl.ds(pl.multiple_of(dev * rows + lo, 16), hi - lo)

        if theirs:
            src = dst = everyone.at[at(place(part, r, 1) if level == 3 else place(part, r + n))]
        else:
            dst = everyone.at[at(place(part, r))]
            src = own.at[pl.ds(lo, hi - lo)] if r == 0 else dst
        return pltpu.make_async_remote_copy(
            src_ref=src, dst_ref=dst, send_sem=ss.at[n * part + r], recv_sem=rs.at[n * part + r],
            device_id=(across(me, 0 if level == 3 else 1 + (part + level) % 3),), device_id_type=MESH)

    doc = Gather(functools.partial(hop, docs_own, docs, (0, 336, 672, 1024), d_sems))
    qry = Gather(functools.partial(hop, q_ref, q_all, (0, 176, 352, 512), q_sems))
    doc.begin()
    docs[pl.ds(pl.multiple_of(me * CHUNK, CHUNK), CHUNK), :] = docs_own[...]
    m = ROWS // SUB_COUNT

    def forward(i, _):
        at = pl.ds(pl.multiple_of(i * m, m), m)
        h = x_ref[at, :]
        for k in range(2):
            for j in TILES:
                cs = slice(j * COLS, (j + 1) * COLS)
                u_ref[:, cs] = gelu(mm(h, w1_ref[k, :, cs])).astype(BF16)
            h = (h.astype(F32) + mm(u_ref[...], w2_ref[k])).astype(BF16)
        q_ref[at, :] = mm(h, p_ref[...]).astype(BF16)
        return 0

    lax.fori_loop(0, SUB_COUNT, forward, 0)
    local = pltpu.make_async_copy(q_ref, q_all.at[pl.ds(pl.multiple_of(me * ROWS, ROWS), ROWS)], local_sem)
    local.start()
    doc.pass_on(2, 0)
    m_ref[...] = jnp.full_like(m_ref, LOW)
    lane = lax.broadcasted_iota(jnp.int32, (ROWS, 128), 1)

    def device_at(k):
        chip = k // 2
        chip = jnp.where(chip == 3, 4, jnp.where(chip == 4, 3, chip))
        flips = 2 * chip + lax.rem(k, 2)
        return me + sum((1 - 2 * bit_of(me, b)) * (1 << b) * lax.rem(flips // (1 << b), 2) for b in range(4))

    def score(k, carry):
        @pl.when(k == 1)
        def _():
            doc.core(0)

        @pl.when(k == 2)
        def _():
            doc.pass_on(1, 0)
            doc.pass_on(0, 0)

        @pl.when(k == 3)
        def _():
            doc.core(1, 2, 4)

        @pl.when(k == 8)
        def _():
            doc.pass_on(1, 1)
            qry.begin()
            doc.pass_on(0, 1, 2)

        @pl.when(k == 9)
        def _():
            doc.core(3, 5, 6)

        @pl.when(k == 14)
        def _():
            doc.pass_on(0, 3)

        @pl.when(k == 15)
        def _():
            doc.core(7)

        top, total = carry
        base = device_at(k) * CHUNK
        marks = m_ref[...]
        for half in range(2):
            rows = docs[pl.ds(pl.multiple_of(base + half * ROWS, ROWS), ROWS), :]
            s = mm(q_ref[...], rows, LAST)
            best = jnp.max(s, axis=1, keepdims=True)
            e = jnp.exp2((s - best) * c)
            e_ref[k, :, half * ROWS:(half + 1) * ROWS] = e
            marks = jnp.where(lane == 2 * k + half, best, marks)
            new_top = jnp.maximum(top, best)
            total = total * jnp.exp2((top - new_top) * c) + jnp.sum(e, axis=1, keepdims=True) * jnp.exp2((best - new_top) * c)
            top = new_top
        m_ref[...] = marks
        return top, total

    top, total = lax.fori_loop(0, ND, score, (jnp.full((ROWS, 1), LOW, F32), jnp.zeros((ROWS, 1), F32)))
    pos = jnp.sum(q_ref[...].astype(F32) * docs_own[0:ROWS, :].astype(F32), axis=1, keepdims=True)
    loss = (top - pos) * inv_tau + jnp.log(total)
    weight = scale / total
    mine_ref[...] = jnp.where(lane == 0, top, jnp.where(lane == 1, weight, loss)).T[0:8, :]
    stat_ref[me] = mine_ref[...]

    def share(p, slot):
        return pltpu.make_async_remote_copy(
            src_ref=mine_ref, dst_ref=stat_ref.at[slot], send_sem=share_send.at[p], recv_sem=share_recv.at[p],
            device_id=(lax.rem(me + p, ND),), device_id_type=MESH)

    for p in range(1, ND):
        share(p, me).start()
    m_ref[...] = jnp.exp2((m_ref[...] - top) * c) * weight
    qry.pass_on(2, 0)

    def weighted(k, half):
        f = jnp.sum(jnp.where(lane == 2 * k + half, m_ref[...], 0.0), axis=1, keepdims=True)
        return e_ref[k, :, half * ROWS:(half + 1) * ROWS] * f

    r = lax.broadcasted_iota(jnp.int32, (ROWS, ROWS), 0)
    col = lax.broadcasted_iota(jnp.int32, (ROWS, ROWS), 1)
    acc[...] = mm((weighted(0, 0) - jnp.where(r == col, scale, 0.0)).astype(BF16), docs_own[0:ROWS, :])
    acc[...] += mm(weighted(0, 1).astype(BF16), docs_own[ROWS:, :])

    def pull(k, _):
        @pl.when(k == 5)
        def _():
            qry.pass_on(1, 0)
            qry.pass_on(0, 0)

        @pl.when(k == 10)
        def _():
            qry.pass_on(1, 1)

        base = device_at(k) * CHUNK
        for half in range(2):
            g_ref[:, half * ROWS:(half + 1) * ROWS] = weighted(k, half).astype(BF16)
        acc[...] += mm(g_ref[...], docs[pl.ds(pl.multiple_of(base, CHUNK), CHUNK), :])
        return 0

    lax.fori_loop(1, ND, pull, 0)
    up_ref[...] = acc[...].astype(BF16)
    qry.pass_on(0, 1, 2, 3)
    qry.core(*range(8))
    for p in range(1, ND):
        share(p, me).wait_send()
        share(p, lax.rem(me + ND - p, ND)).wait_recv()
    doc.drain()
    qry.drain()
    local.wait()


def gather_rows(tau, docs_own, x, w1, w2, p):
    vmem = pl.BlockSpec(memory_space=pltpu.VMEM)
    return pl.pallas_call(
        gather_kernel,
        out_shape=[
            jax.ShapeDtypeStruct((ROWS, WIDTH), BF16),
            jax.ShapeDtypeStruct((ND, 8, ROWS), F32),
            jax.ShapeDtypeStruct((BATCH, WIDTH), BF16),
        ],
        in_specs=[pl.BlockSpec(memory_space=pltpu.SMEM)] + [vmem] * 5,
        out_specs=[vmem, vmem, pl.BlockSpec(memory_space=pl.ANY)],
        scratch_shapes=[
            pltpu.VMEM((2 * BATCH, WIDTH), BF16),
            pltpu.VMEM((ND, ROWS, CHUNK), F32),
            pltpu.VMEM((ROWS, 128), F32),
            pltpu.VMEM((ROWS, CHUNK), BF16),
            pltpu.VMEM((ROWS, WIDTH), F32),
            pltpu.VMEM((ROWS // SUB_COUNT, FFN), BF16),
            pltpu.VMEM((ROWS, WIDTH), BF16),
            pltpu.VMEM((8, ROWS), F32),
        ] + HOP_SEMS + HOP_SEMS + [pltpu.SemaphoreType.DMA((ND,)), pltpu.SemaphoreType.DMA((ND,)), pltpu.SemaphoreType.DMA],
        compiler_params=pltpu.CompilerParams(collective_id=0, has_side_effects=True, vmem_limit_bytes=VMEM_MAX),
        name="gather_rows",
    )(tau, docs_own, x, w1, w2, p)


def tail_kernel(tau_ref, stat_ref, own_ref, x_ref, w1_ref, w2_ref, p_ref, grads_q, q_ref, out_q, out_d,
                q_buf, g_ref, up_ref, grads, u_ref, s_ref, h_ref, dl_ref, held, q_sem, load_sems, *rest):
    me = lax.axis_index("data")
    inv_tau = 1.0 / tau_ref[0]
    c = inv_tau * LOG2E
    scale = inv_tau / BATCH
    places = mine, partner, peers = sum_places(me)
    barrier = pltpu.get_barrier_semaphore()
    for b in range(4):
        pl.semaphore_signal(barrier, inc=1, device_id=(peers[b],), device_id_type=MESH)
    pl.semaphore_wait(barrier, 4)
    queries = pltpu.make_async_copy(q_ref, q_buf, q_sem)
    queries.start()

    def load(p, r):
        k = 8 * p + r
        return pltpu.make_async_copy(grads_q.at[mine[k]], held.at[k], load_sems.at[k])

    sum_q = DeviceSum(places, lambda p, r: held.at[8 * p + r], lambda p, r: grads_q.at[partner[8 * p + r]], out_q,
                      rest[0:4], rest[8:25], load)
    sum_d = DeviceSum(places, lambda p, r: grads.at[mine[8 * p + r]], lambda p, r: grads.at[partner[8 * p + r]], out_d,
                      rest[4:8], rest[25:42])
    sum_q.start()

    def rows_of(k):
        return pl.ds(pl.multiple_of(lax.rem(me + k, ND) * ROWS, ROWS), ROWS)

    def probs(k):
        j = lax.rem(me + k, ND)
        s = mm(own_ref[...], q_buf[rows_of(k), :], LAST)
        return jnp.exp2((s - stat_ref[j, 0:1, :]) * c) * stat_ref[j, 1:2, :]

    grads[...] = jnp.zeros_like(grads)
    queries.wait()
    row = lax.broadcasted_iota(jnp.int32, (CHUNK, ROWS), 0)
    col = lax.broadcasted_iota(jnp.int32, (CHUNK, ROWS), 1)
    up_ref[...] = mm((probs(0) - jnp.where(row == col, scale, 0.0)).astype(BF16), q_buf[rows_of(0), :])
    sum_q.swapped(FAR)

    def columns(i, _):
        @pl.when(i == 1)
        def _():
            sum_q.swapped(NEAR)

        @pl.when(i == 2)
        def _():
            sum_q.second(3)

        @pl.when(i == 3)
        def _():
            sum_q.second(2)

        for n in range(3):
            k = 3 * i + n + 1
            g_ref[n % 2] = probs(k).astype(BF16)
            up_ref[...] += mm(g_ref[n % 2], q_buf[rows_of(k), :])
        return 0

    lax.fori_loop(0, 5, columns, 0)
    m = CHUNK // SUB_COUNT

    def add(block, value):
        grads[block * WIDTH:(block + 1) * WIDTH, :] += value

    def backward(i, _):
        @pl.when(i == 2)
        def _():
            sum_q.finish()

        @pl.when(i == 3)
        def _():
            sum_q.gather.pass_on(2, 0)

        def middle():
            @pl.when(i == 0)
            def _():
                sum_q.third()

        at = pl.ds(pl.multiple_of(i * m, m), m)
        backward_rows(x_ref[at, :], up_ref[at, :].astype(BF16), w1_ref, w2_ref, p_ref, add, u_ref, s_ref, h_ref, dl_ref, middle)
        return 0

    lax.fori_loop(0, SUB_COUNT, backward, 0)
    sum_d.start()
    sum_q.gather.pass_on(1, 0)
    sum_d.swapped(FAR)
    sum_q.gather.pass_on(1, 1)
    sum_d.swapped(NEAR)
    sum_q.gather.pass_on(0, 0, 1)
    sum_d.second(3)
    sum_q.gather.pass_on(0, 2)
    sum_d.second(2)
    sum_q.gather.pass_on(0, 3)
    sum_d.third()
    sum_d.finish()
    sum_d.gather.pass_on(2, 0)
    sum_d.gather.pass_on(1, 0, 1)
    sum_d.gather.pass_on(0, *range(4))
    sum_q.close()
    sum_d.close()


def tail(tau, stats, own, x, w1, w2, p, grads_q, q_all):
    vmem, hbm = pl.BlockSpec(memory_space=pltpu.VMEM), pl.BlockSpec(memory_space=pl.ANY)
    packed = jax.ShapeDtypeStruct((BLOCKS * WIDTH, WIDTH), F32)
    m = CHUNK // SUB_COUNT
    return pl.pallas_call(
        tail_kernel,
        out_shape=[packed, packed],
        in_specs=[pl.BlockSpec(memory_space=pltpu.SMEM)] + [vmem] * 6 + [hbm, hbm],
        out_specs=[hbm, hbm],
        scratch_shapes=[
            pltpu.VMEM((BATCH, WIDTH), BF16),
            pltpu.VMEM((2, CHUNK, ROWS), BF16),
            pltpu.VMEM((CHUNK, WIDTH), F32),
            pltpu.VMEM((BLOCKS * WIDTH, WIDTH), F32),
            pltpu.VMEM((2, m, FFN), BF16),
            pltpu.VMEM((2, m, FFN), F32),
            pltpu.VMEM((3, m, WIDTH), BF16),
            pltpu.VMEM((m, FFN), BF16),
            pltpu.VMEM((24, PIECE, WIDTH), F32),
            pltpu.SemaphoreType.DMA,
            pltpu.SemaphoreType.DMA((24,)),
        ] + SUM_BUFS + SUM_BUFS + SUM_SEMS + SUM_SEMS,
        compiler_params=pltpu.CompilerParams(collective_id=1, has_side_effects=True, vmem_limit_bytes=VMEM_MAX),
        name="tail",
    )(tau, stats, own, x, w1, w2, p, grads_q, q_all)


def local_step(q_loc, d_loc, temperature, q_w1, q_w2, q_proj, d_w1, d_w2, d_proj):
    tau = temperature.reshape(1)
    d_rows = d_loc.reshape(CHUNK, WIDTH)
    d_reps = tower_forward(d_rows, d_w1, d_w2, d_proj)
    q_up, stats, q_all = gather_rows(tau, d_reps, q_loc, q_w1, q_w2, q_proj)
    loss = jnp.sum(stats[:, 2, :]) / BATCH
    q_grads = tower_backward(q_loc, q_up, q_w1, q_w2, q_proj)
    q_sum, d_sum = tail(tau, stats, d_reps, d_rows, d_w1, d_w2, d_proj, q_grads.reshape(BLOCKS * WIDTH, WIDTH), q_all)
    shapes = [a.shape for a in (q_w1, q_w2, q_proj, d_w1, d_w2, d_proj)]
    packed = (BLOCKS, WIDTH, WIDTH)
    return (loss, *unpack(q_sum.reshape(packed), d_sum.reshape(packed), shapes))


def solution(mesh):
    specs_in = (P("data", None), P(None, "data", None), P(), P(), P(), P(), P(), P(), P())
    specs_out = (P(), P(), P(), P(), P(), P(), P())
    return jax.shard_map(local_step, mesh=mesh, in_specs=specs_in, out_specs=specs_out, check_vma=False)
```

```python
import functools

import jax
import jax.numpy as jnp
import numpy as np
from jax import lax
from jax.experimental import pallas as pl
from jax.experimental.pallas import tpu as pltpu
from jax.sharding import PartitionSpec as P

SUB_COUNT = 4
ND = 16
ROWS = 512
WIDTH = 384
FFN = 1536
BATCH = ROWS * ND
CHUNK = 2 * ROWS
BLOCKS = 17
HALF_ROWS = BLOCKS * WIDTH // 2
PART_ROWS = HALF_ROWS // 3
PIECE = PART_ROWS // 8
PARTS = range(3)
NEAR, FAR = range(3, -1, -1), range(7, 3, -1)
HOPS = (4, 2, 1, 8)
COLS = 512
TILES = range(FFN // COLS)
MESH = pl.DeviceIdType.MESH
VMEM_MAX = 67_043_328
F32, BF16 = jnp.float32, jnp.bfloat16
K0 = float(np.sqrt(2.0 / np.pi).astype(np.float32))
LOW = -3.0e38
LOG2E = float(1.0 / np.log(2.0))

LAST = (((1,), (1,)), ((), ()))
FIRST = (((0,), (0,)), ((), ()))
NORMAL = (((1,), (0,)), ((), ()))


def mm(a, b, dims=NORMAL):
    return lax.dot_general(a, b, dims, preferred_element_type=F32)


def gelu(a):
    return a * (0.5 * (1.0 + jnp.tanh(K0 * (a + 0.044715 * (a * a * a)))))


def gelu_and_slope(a):
    sq = a * a
    t = jnp.tanh(K0 * (a + 0.044715 * (a * sq)))
    cdf = 0.5 * (1.0 + t)
    slope = cdf + a * (0.5 * (1.0 - t * t)) * (K0 + (3.0 * 0.044715 * K0) * sq)
    return a * cdf, slope


def fetches(srcs, dsts, sems):
    return [pltpu.make_async_copy(src, dst, sems.at[i]) for i, (src, dst) in enumerate(zip(srcs, dsts))]


def forward_rows(x_ref, y_ref, w1_ref, w2_ref, p_ref, u_ref):
    m = x_ref.shape[0] // SUB_COUNT

    def step(i, _):
        at = pl.ds(pl.multiple_of(i * m, m), m)
        h = x_ref[at, :]
        for k in range(2):
            for j in TILES:
                cs = slice(j * COLS, (j + 1) * COLS)
                u_ref[:, cs] = gelu(mm(h, w1_ref[k, :, cs])).astype(BF16)
            h = (h.astype(F32) + mm(u_ref[...], w2_ref[k])).astype(BF16)
        y_ref[at, :] = mm(h, p_ref[...]).astype(BF16)
        return 0

    lax.fori_loop(0, SUB_COUNT, step, 0)


WEIGHTS = [
    pltpu.VMEM((2, WIDTH, FFN), BF16), pltpu.VMEM((2, FFN, WIDTH), BF16), pltpu.VMEM((WIDTH, WIDTH), BF16),
    pltpu.SemaphoreType.DMA((3,))]
INNER, OUTER = pl.BlockSpec(memory_space=pltpu.VMEM), pl.BlockSpec(memory_space=pltpu.HBM)
SCALAR = pl.BlockSpec(memory_space=pltpu.SMEM)


def forward_kernel(x_ref, w1_ref, w2_ref, p_ref, y_ref, u_ref, w1, w2, p, w_sems):
    loads = fetches((w1_ref, w2_ref, p_ref), (w1, w2, p), w_sems)
    for load in loads:
        load.start()
    for load in loads:
        load.wait()
    forward_rows(x_ref, y_ref, w1, w2, p, u_ref)


def tower_forward(rows, w1, w2, p):
    return pl.pallas_call(
        forward_kernel,
        out_shape=jax.ShapeDtypeStruct(rows.shape, BF16),
        in_specs=[INNER] + [OUTER] * 3,
        out_specs=INNER,
        scratch_shapes=[pltpu.VMEM((rows.shape[0] // SUB_COUNT, FFN), BF16)] + WEIGHTS,
        compiler_params=pltpu.CompilerParams(vmem_limit_bytes=VMEM_MAX),
        name="tower_forward",
    )(rows, w1, w2, p)


def backward_rows(x, g, w1_ref, w2_ref, p_ref, add, u_ref, s_ref, h_ref, dl_ref, middle=None):
    h_ref[0] = x
    for k in range(2):
        h = h_ref[k]
        for c in TILES:
            cs = slice(c * COLS, (c + 1) * COLS)
            act, slope = gelu_and_slope(mm(h, w1_ref[k, :, cs]))
            u_ref[k, :, cs] = act.astype(BF16)
            s_ref[k, :, cs] = slope
        h_ref[k + 1] = (h.astype(F32) + mm(u_ref[k], w2_ref[k])).astype(BF16)
    if middle is not None:
        middle()
    add(16, mm(h_ref[2], g, FIRST))
    e = mm(g, p_ref[...], LAST)
    for k in (1, 0):
        eb = e.astype(BF16)
        for c in range(4):
            add(8 + 4 * k + c, mm(u_ref[k, :, c * WIDTH:(c + 1) * WIDTH], eb, FIRST))
        for c in TILES:
            cs = slice(c * COLS, (c + 1) * COLS)
            dl_ref[:, cs] = (s_ref[k, :, cs] * mm(eb, w2_ref[k, cs, :], LAST)).astype(BF16)
        for c in range(2):
            part = mm(h_ref[k], dl_ref[:, 2 * c * WIDTH:2 * (c + 1) * WIDTH], FIRST)
            add(4 * k + 2 * c, part[:, :WIDTH])
            add(4 * k + 2 * c + 1, part[:, WIDTH:])
        if k == 1:
            e = e + mm(dl_ref[...], w1_ref[k], LAST)


def unpack_kernel(q_ref, d_ref, *refs):
    outs, hold, load, store = refs[:6], refs[6], refs[7], refs[8]

    def place(j):
        w1, w2, p = outs[3 * (j // BLOCKS):3 * (j // BLOCKS) + 3]
        n = j % BLOCKS
        if n < 8:
            return w1.at[n // 4, :, pl.ds(n % 4 * WIDTH, WIDTH)]
        if n < 16:
            return w2.at[(n - 8) // 4, pl.ds(n % 4 * WIDTH, WIDTH), :]
        return p

    def fetch(j):
        return pltpu.make_async_copy((q_ref, d_ref)[j // BLOCKS].at[j % BLOCKS], hold.at[j], load.at[j])

    def put(j):
        return pltpu.make_async_copy(hold.at[j], place(j), store.at[j])

    for j in range(2 * BLOCKS):
        fetch(j).start()
    for j in range(2 * BLOCKS):
        fetch(j).wait()
        put(j).start()
    for j in range(2 * BLOCKS):
        put(j).wait()


def unpack(q_blocks, d_blocks, shapes):
    return pl.pallas_call(
        unpack_kernel,
        out_shape=[jax.ShapeDtypeStruct(a, F32) for a in shapes],
        in_specs=[OUTER, OUTER],
        out_specs=[OUTER] * 6,
        scratch_shapes=[
            pltpu.VMEM((2 * BLOCKS, WIDTH, WIDTH), F32),
            pltpu.SemaphoreType.DMA((2 * BLOCKS,)),
            pltpu.SemaphoreType.DMA((2 * BLOCKS,)),
        ],
        compiler_params=pltpu.CompilerParams(vmem_limit_bytes=24 << 20),
        name="unpack",
    )(q_blocks, d_blocks)


def bit_of(me, b):
    return lax.rem(me // (1 << b), 2)


def across(me, b):
    return me + (1 - 2 * bit_of(me, b)) * (1 << b)


def sum_places(me):
    core, bits = bit_of(me, 0), [bit_of(me, b) for b in (1, 2, 3)]
    mine, partner = [], []
    for p in PARTS:
        side = [(bits[(p + i) % 3] * (4 >> i) * PIECE, (1 - bits[(p + i) % 3]) * (4 >> i) * PIECE) for i in range(3)]
        for r in range(8):
            at = p * PART_ROWS + side[0][r >> 2] + side[1][(r >> 1) & 1] + side[2][r & 1]
            mine.append(pl.ds(pl.multiple_of(core * HALF_ROWS + at, 8), PIECE))
            partner.append(pl.ds(pl.multiple_of((1 - core) * HALF_ROWS + at, 8), PIECE))
    return mine, partner, [across(me, b) for b in range(4)]


class Gather:
    def __init__(self, copy):
        self.copy = copy

    def begin(self):
        for level in (2, 1, 0, 3):
            for p in PARTS:
                self.copy(p, 0, level).start()

    def pass_on(self, level, *rs):
        for r in rs:
            for p in PARTS:
                self.copy(p, r, level, True).wait_recv()
                for lower in (*range(level - 1, -1, -1), 3):
                    self.copy(p, r + HOPS[level], lower).start()

    def core(self, *rs):
        for r in rs:
            for p in PARTS:
                self.copy(p, r, 3, True).wait_recv()

    def drain(self):
        for level, n in enumerate(HOPS):
            for r in range(n):
                for p in PARTS:
                    self.copy(p, r, level).wait_send()


def place(me, part, r, other=0):
    dev = across(me, 0) if other else me
    for i in range(3):
        if (r >> (2 - i)) & 1:
            dev = dev + (1 - 2 * bit_of(me, 1 + (part + i) % 3)) * (1 << (1 + (part + i) % 3))
    return dev


def hop(me, own, everyone, cuts, sem, part, r, level, theirs=False):
    n = HOPS[level]
    ss, rs = sem[2 * level], sem[2 * level + 1]
    rows, lo, hi = own.shape[0], cuts[part], cuts[part + 1]

    def at(dev):
        return pl.ds(pl.multiple_of(dev * rows + lo, 16), hi - lo)

    if theirs:
        src = dst = everyone.at[at(place(me, part, r, 1) if level == 3 else place(me, part, r + n))]
    else:
        dst = everyone.at[at(place(me, part, r))]
        src = own.at[pl.ds(lo, hi - lo)] if r == 0 else dst
    return pltpu.make_async_remote_copy(
        src_ref=src, dst_ref=dst, send_sem=ss.at[n * part + r], recv_sem=rs.at[n * part + r],
        device_id=(across(me, 0 if level == 3 else 1 + (part + level) % 3),), device_id_type=MESH)


HOP_SEMS = [pltpu.SemaphoreType.DMA((3 * n,)) for n in HOPS for _ in range(2)]


class DeviceSum:
    def __init__(self, places, own, other, out, bufs, sems, load=None):
        self.mine, self.partner, self.peers = places
        self.own, self.other, self.out, self.load = own, other, out, load
        self.bufs, self.sems = bufs, sems
        self.gather = Gather(self.back)

    def copy(self, src, dst, level, k, b):
        return pltpu.make_async_remote_copy(
            src_ref=src, dst_ref=dst, send_sem=self.sems[2 * level].at[k], recv_sem=self.sems[2 * level + 1].at[k],
            device_id=(self.peers[b],), device_id_type=MESH)

    def swap(self, p, r):
        return self.copy(self.other(p, r), self.bufs[0].at[8 * p + r], 0, 8 * p + r, 0)

    def link(self, p, r, level):
        n = HOPS[level]
        return self.copy(self.own(p, n + r), self.bufs[1 + level].at[n * p + r], 1 + level, n * p + r, 1 + (p + level) % 3)

    def back(self, p, r, level, theirs=False):
        n = HOPS[level]
        if theirs and level == 3:
            dst = self.out.at[self.partner[8 * p + r]]
        else:
            dst = self.out.at[self.mine[8 * p + (r + n if theirs else r)]]
        src = self.own(p, 0) if r == 0 and not theirs else dst
        return self.copy(src, dst, 4 + level, n * p + r, 0 if level == 3 else 1 + (p + level) % 3)

    def keep(self, p):
        return pltpu.make_async_copy(self.own(p, 0), self.out.at[self.mine[8 * p]], self.sems[16].at[p])

    def plus(self, p, r, *terms):
        ref = self.own(p, r)
        value = ref[...]
        for level, k in terms:
            value = value + self.bufs[level][k]
        ref[...] = value

    def start(self):
        for r in reversed(range(8)):
            for p in PARTS:
                if self.load is not None:
                    self.load(p, r).start()
                self.swap(p, r).start()

    def swapped(self, rs):
        for r in rs:
            for p in PARTS:
                if self.load is not None:
                    self.load(p, r).wait()
                self.swap(p, r).wait_recv()
                self.plus(p, r, (0, 8 * p + r))
                if r >= 4:
                    self.link(p, r - 4, 0).start()

    def second(self, r):
        for p in PARTS:
            self.link(p, r, 0).wait_recv()
            self.plus(p, r, (1, 4 * p + r))
            self.link(p, r - 2, 1).start()

    def third(self):
        for p in PARTS:
            self.link(p, 1, 0).wait_recv()
            self.link(p, 1, 1).wait_recv()
            self.plus(p, 1, (1, 4 * p + 1), (2, 2 * p + 1))
            self.link(p, 0, 2).start()

    def finish(self):
        for p in PARTS:
            self.link(p, 0, 0).wait_recv()
            self.link(p, 0, 1).wait_recv()
            self.link(p, 0, 2).wait_recv()
            self.plus(p, 0, (1, 4 * p), (2, 2 * p), (3, p))
        self.gather.begin()
        for p in PARTS:
            self.keep(p).start()

    def close(self):
        self.gather.core(*range(8))
        self.gather.drain()
        for p in PARTS:
            for r in range(8):
                self.swap(p, r).wait_send()
            for level in PARTS:
                for r in range(HOPS[level]):
                    self.link(p, r, level).wait_send()
            self.keep(p).wait()


SUM_BUFS = [pltpu.VMEM((n, PIECE, WIDTH), F32) for n in (24, 12, 6, 3)]
SUM_SEMS = [pltpu.SemaphoreType.DMA((n,)) for n in (24, 12, 6, 3) for _ in range(2)] + HOP_SEMS + [pltpu.SemaphoreType.DMA((3,))]


def gather_kernel(tau_ref, docs_own, x_ref, w1_ref, w2_ref, p_ref, up_ref, stat_ref, q_ref, docs, e_ref, m_ref, g_ref, acc, u_ref,
                  mine_ref, w1, w2, p_w, w_sems, share_send, share_recv, *d_sems):
    me = lax.axis_index("data")
    loads = fetches((w1_ref, w2_ref, p_ref), (w1, w2, p_w), w_sems)
    for load in loads:
        load.start()
    inv_tau = 1.0 / tau_ref[0]
    c = inv_tau * LOG2E
    scale = inv_tau / BATCH
    barrier = pltpu.get_barrier_semaphore()
    for p in range(1, ND):
        pl.semaphore_signal(barrier, inc=1, device_id=(lax.rem(me + p, ND),), device_id_type=MESH)
    pl.semaphore_wait(barrier, ND - 1)

    doc = Gather(functools.partial(hop, me, docs_own, docs, (0, 336, 672, 1024), d_sems))
    doc.begin()
    docs[pl.ds(pl.multiple_of(me * CHUNK, CHUNK), CHUNK), :] = docs_own[...]
    for load in loads:
        load.wait()
    forward_rows(x_ref, q_ref, w1, w2, p_w, u_ref)
    doc.pass_on(2, 0)
    m_ref[...] = jnp.full_like(m_ref, LOW)
    lane = lax.broadcasted_iota(jnp.int32, (ROWS, 128), 1)

    def device_at(k):
        chip = k // 2
        chip = jnp.where(chip == 3, 4, jnp.where(chip == 4, 3, chip))
        flips = 2 * chip + lax.rem(k, 2)
        return me + sum((1 - 2 * bit_of(me, b)) * (1 << b) * lax.rem(flips // (1 << b), 2) for b in range(4))

    def score(k, carry):
        @pl.when(k == 1)
        def _():
            doc.core(0)

        @pl.when(k == 2)
        def _():
            doc.pass_on(1, 0)
            doc.pass_on(0, 0)

        @pl.when(k == 3)
        def _():
            doc.core(1, 2, 4)

        @pl.when(k == 8)
        def _():
            doc.pass_on(1, 1)
            doc.pass_on(0, 1, 2)

        @pl.when(k == 9)
        def _():
            doc.core(3, 5, 6)

        @pl.when(k == 14)
        def _():
            doc.pass_on(0, 3)

        @pl.when(k == 15)
        def _():
            doc.core(7)

        top, total = carry
        base = device_at(k) * CHUNK
        marks = m_ref[...]
        for half in range(2):
            rows = docs[pl.ds(pl.multiple_of(base + half * ROWS, ROWS), ROWS), :]
            s = mm(q_ref[...], rows, LAST)
            best = jnp.max(s, axis=1, keepdims=True)
            e = jnp.exp2((s - best) * c)
            e_ref[k, :, half * ROWS:(half + 1) * ROWS] = e
            marks = jnp.where(lane == 2 * k + half, best, marks)
            new_top = jnp.maximum(top, best)
            total = total * jnp.exp2((top - new_top) * c) + jnp.sum(e, axis=1, keepdims=True) * jnp.exp2((best - new_top) * c)
            top = new_top
        m_ref[...] = marks
        return top, total

    top, total = lax.fori_loop(0, ND, score, (jnp.full((ROWS, 1), LOW, F32), jnp.zeros((ROWS, 1), F32)))
    pos = jnp.sum(q_ref[...].astype(F32) * docs_own[0:ROWS, :].astype(F32), axis=1, keepdims=True)
    loss = (top - pos) * inv_tau + jnp.log(total)
    weight = scale / total
    mine_ref[...] = jnp.where(lane == 0, top, jnp.where(lane == 1, weight, loss)).T[0:8, :]
    stat_ref[me] = mine_ref[...]

    def share(p, slot):
        return pltpu.make_async_remote_copy(
            src_ref=mine_ref, dst_ref=stat_ref.at[slot], send_sem=share_send.at[p], recv_sem=share_recv.at[p],
            device_id=(lax.rem(me + p, ND),), device_id_type=MESH)

    for p in range(1, ND):
        share(p, me).start()
    m_ref[...] = jnp.exp2((m_ref[...] - top) * c) * weight

    def weighted(k, half):
        f = jnp.sum(jnp.where(lane == 2 * k + half, m_ref[...], 0.0), axis=1, keepdims=True)
        return e_ref[k, :, half * ROWS:(half + 1) * ROWS] * f

    r = lax.broadcasted_iota(jnp.int32, (ROWS, ROWS), 0)
    col = lax.broadcasted_iota(jnp.int32, (ROWS, ROWS), 1)
    acc[...] = mm((weighted(0, 0) - jnp.where(r == col, scale, 0.0)).astype(BF16), docs_own[0:ROWS, :])
    acc[...] += mm(weighted(0, 1).astype(BF16), docs_own[ROWS:, :])

    def pull(k, _):
        base = device_at(k) * CHUNK
        for half in range(2):
            g_ref[:, half * ROWS:(half + 1) * ROWS] = weighted(k, half).astype(BF16)
        acc[...] += mm(g_ref[...], docs[pl.ds(pl.multiple_of(base, CHUNK), CHUNK), :])
        return 0

    lax.fori_loop(1, ND, pull, 0)
    up_ref[...] = acc[...].astype(BF16)
    for p in range(1, ND):
        share(p, me).wait_send()
        share(p, lax.rem(me + ND - p, ND)).wait_recv()
    doc.drain()


def gather_rows(tau, docs_own, x, w1, w2, p):
    mine = jax.ShapeDtypeStruct((ROWS, WIDTH), BF16)
    return pl.pallas_call(
        gather_kernel,
        out_shape=[mine, jax.ShapeDtypeStruct((ND, 8, ROWS), F32), mine],
        in_specs=[SCALAR, INNER, INNER] + [OUTER] * 3,
        out_specs=[INNER] * 3,
        scratch_shapes=[
            pltpu.VMEM((2 * BATCH, WIDTH), BF16),
            pltpu.VMEM((ND, ROWS, CHUNK), F32),
            pltpu.VMEM((ROWS, 128), F32),
            pltpu.VMEM((ROWS, CHUNK), BF16),
            pltpu.VMEM((ROWS, WIDTH), F32),
            pltpu.VMEM((ROWS // SUB_COUNT, FFN), BF16),
            pltpu.VMEM((8, ROWS), F32),
        ] + WEIGHTS + [pltpu.SemaphoreType.DMA((ND,)), pltpu.SemaphoreType.DMA((ND,))] + HOP_SEMS,
        compiler_params=pltpu.CompilerParams(collective_id=0, has_side_effects=True, vmem_limit_bytes=VMEM_MAX),
        name="gather_rows",
    )(tau, docs_own, x, w1, w2, p)


def greet(peers):
    barrier = pltpu.get_barrier_semaphore()
    for peer in peers:
        pl.semaphore_signal(barrier, inc=1, device_id=(peer,), device_id_type=MESH)
    pl.semaphore_wait(barrier, len(peers))


def query_kernel(q_ref, x_ref, up_ref, w1_ref, w2_ref, p_ref, out_ref, q_all, u_ref, s_ref, h_ref, dl_ref, w1, w2, p, w_sems,
                 local_sem, *sems):
    me = lax.axis_index("data")
    loads = fetches((w1_ref, w2_ref, p_ref), (w1, w2, p), w_sems)
    for load in loads:
        load.start()
    greet([across(me, b) for b in range(4)])
    qry = Gather(functools.partial(hop, me, q_ref, q_all, (0, 176, 352, 512), sems))
    qry.begin()
    local = pltpu.make_async_copy(q_ref, q_all.at[pl.ds(pl.multiple_of(me * ROWS, ROWS), ROWS)], local_sem)
    local.start()
    out_ref[...] = jnp.zeros_like(out_ref)
    for load in loads:
        load.wait()
    m = ROWS // SUB_COUNT

    def add(block, value):
        out_ref[block * WIDTH:(block + 1) * WIDTH, :] += value

    def step(i, _):
        @pl.when(i == 1)
        def _():
            qry.pass_on(2, 0)

        @pl.when(i == 2)
        def _():
            qry.pass_on(1, 0)
            qry.pass_on(0, 0)

        @pl.when(i == 3)
        def _():
            qry.pass_on(1, 1)

        at = pl.ds(pl.multiple_of(i * m, m), m)
        backward_rows(x_ref[at, :], up_ref[at, :], w1, w2, p, add, u_ref, s_ref, h_ref, dl_ref)
        return 0

    lax.fori_loop(0, SUB_COUNT, step, 0)
    qry.pass_on(0, 1, 2, 3)
    qry.core(*range(8))
    qry.drain()
    local.wait()


def backward_scratch(m):
    return [pltpu.VMEM((2, m, FFN), BF16), pltpu.VMEM((2, m, FFN), F32), pltpu.VMEM((3, m, WIDTH), BF16), pltpu.VMEM((m, FFN), BF16)]


PACKED = jax.ShapeDtypeStruct((BLOCKS * WIDTH, WIDTH), F32)


def query_backward(q, x, up, w1, w2, p):
    return pl.pallas_call(
        query_kernel,
        out_shape=[PACKED, jax.ShapeDtypeStruct((BATCH, WIDTH), BF16)],
        in_specs=[INNER] * 3 + [OUTER] * 3,
        out_specs=[INNER, OUTER],
        scratch_shapes=backward_scratch(ROWS // SUB_COUNT) + WEIGHTS + [pltpu.SemaphoreType.DMA] + HOP_SEMS,
        compiler_params=pltpu.CompilerParams(collective_id=2, has_side_effects=True, vmem_limit_bytes=VMEM_MAX),
        name="query_backward",
    )(q, x, up, w1, w2, p)


def tail_kernel(tau_ref, stat_ref, own_ref, x_ref, w1_ref, w2_ref, p_ref, grads_q, q_ref, out_q, out_d,
                q_buf, g_ref, up_ref, grads, u_ref, s_ref, h_ref, dl_ref, w1, w2, p_w, w_sems, held, q_sem, load_sems, *rest):
    me = lax.axis_index("data")
    loads = fetches((w1_ref, w2_ref, p_ref), (w1, w2, p_w), w_sems)
    inv_tau = 1.0 / tau_ref[0]
    c = inv_tau * LOG2E
    scale = inv_tau / BATCH
    places = mine, partner, peers = sum_places(me)
    greet(peers)
    queries = pltpu.make_async_copy(q_ref, q_buf, q_sem)
    queries.start()

    def load(p, r):
        k = 8 * p + r
        return pltpu.make_async_copy(grads_q.at[mine[k]], held.at[k], load_sems.at[k])

    sum_q = DeviceSum(places, lambda p, r: held.at[8 * p + r], lambda p, r: grads_q.at[partner[8 * p + r]], out_q,
                      rest[0:4], rest[8:25], load)
    sum_d = DeviceSum(places, lambda p, r: grads.at[mine[8 * p + r]], lambda p, r: grads.at[partner[8 * p + r]], out_d,
                      rest[4:8], rest[25:42])
    sum_q.start()
    for load in loads:
        load.start()

    def rows_of(k):
        return pl.ds(pl.multiple_of(lax.rem(me + k, ND) * ROWS, ROWS), ROWS)

    def probs(k):
        j = lax.rem(me + k, ND)
        s = mm(own_ref[...], q_buf[rows_of(k), :], LAST)
        return jnp.exp2((s - stat_ref[j, 0:1, :]) * c) * stat_ref[j, 1:2, :]

    grads[...] = jnp.zeros_like(grads)
    queries.wait()
    row = lax.broadcasted_iota(jnp.int32, (CHUNK, ROWS), 0)
    col = lax.broadcasted_iota(jnp.int32, (CHUNK, ROWS), 1)
    up_ref[...] = mm((probs(0) - jnp.where(row == col, scale, 0.0)).astype(BF16), q_buf[rows_of(0), :])
    sum_q.swapped(FAR)

    def columns(i, _):
        @pl.when(i == 1)
        def _():
            sum_q.swapped(NEAR)

        @pl.when(i == 2)
        def _():
            sum_q.second(3)

        @pl.when(i == 3)
        def _():
            sum_q.second(2)

        for n in range(3):
            k = 3 * i + n + 1
            g_ref[n % 2] = probs(k).astype(BF16)
            up_ref[...] += mm(g_ref[n % 2], q_buf[rows_of(k), :])
        return 0

    lax.fori_loop(0, 5, columns, 0)
    for load in loads:
        load.wait()
    m = CHUNK // SUB_COUNT

    def add(block, value):
        grads[block * WIDTH:(block + 1) * WIDTH, :] += value

    def backward(i, _):
        @pl.when(i == 2)
        def _():
            sum_q.finish()

        @pl.when(i == 3)
        def _():
            sum_q.gather.pass_on(2, 0)

        def middle():
            @pl.when(i == 0)
            def _():
                sum_q.third()

        at = pl.ds(pl.multiple_of(i * m, m), m)
        backward_rows(x_ref[at, :], up_ref[at, :].astype(BF16), w1, w2, p_w, add, u_ref, s_ref, h_ref, dl_ref, middle)
        return 0

    lax.fori_loop(0, SUB_COUNT, backward, 0)
    sum_d.start()
    sum_q.gather.pass_on(1, 0)
    sum_d.swapped(FAR)
    sum_q.gather.pass_on(1, 1)
    sum_d.swapped(NEAR)
    sum_q.gather.pass_on(0, 0, 1)
    sum_d.second(3)
    sum_q.gather.pass_on(0, 2)
    sum_d.second(2)
    sum_q.gather.pass_on(0, 3)
    sum_d.third()
    sum_d.finish()
    sum_d.gather.pass_on(2, 0)
    sum_d.gather.pass_on(1, 0, 1)
    sum_d.gather.pass_on(0, *range(4))
    sum_q.close()
    sum_d.close()


def tail(tau, stats, own, x, w1, w2, p, grads_q, q_all):
    return pl.pallas_call(
        tail_kernel,
        out_shape=[PACKED, PACKED],
        in_specs=[SCALAR] + [INNER] * 3 + [OUTER] * 5,
        out_specs=[OUTER, OUTER],
        scratch_shapes=[
            pltpu.VMEM((BATCH, WIDTH), BF16),
            pltpu.VMEM((2, CHUNK, ROWS), BF16),
            pltpu.VMEM((CHUNK, WIDTH), F32),
            pltpu.VMEM(PACKED.shape, F32),
        ] + backward_scratch(CHUNK // SUB_COUNT) + WEIGHTS + [
            pltpu.VMEM((24, PIECE, WIDTH), F32),
            pltpu.SemaphoreType.DMA,
            pltpu.SemaphoreType.DMA((24,)),
        ] + SUM_BUFS + SUM_BUFS + SUM_SEMS + SUM_SEMS,
        compiler_params=pltpu.CompilerParams(collective_id=1, has_side_effects=True, vmem_limit_bytes=VMEM_MAX),
        name="tail",
    )(tau, stats, own, x, w1, w2, p, grads_q, q_all)


def local_step(q_loc, d_loc, temperature, q_w1, q_w2, q_proj, d_w1, d_w2, d_proj):
    tau = temperature.reshape(1)
    d_rows = d_loc.reshape(CHUNK, WIDTH)
    d_reps = tower_forward(d_rows, d_w1, d_w2, d_proj)
    q_up, stats, q_reps = gather_rows(tau, d_reps, q_loc, q_w1, q_w2, q_proj)
    loss = jnp.sum(stats[:, 2, :]) / BATCH
    q_grads, q_all = query_backward(q_reps, q_loc, q_up, q_w1, q_w2, q_proj)
    q_sum, d_sum = tail(tau, stats, d_reps, d_rows, d_w1, d_w2, d_proj, q_grads, q_all)
    shapes = [a.shape for a in (q_w1, q_w2, q_proj, d_w1, d_w2, d_proj)]
    packed = (BLOCKS, WIDTH, WIDTH)
    return (loss, *unpack(q_sum.reshape(packed), d_sum.reshape(packed), shapes))


def solution(mesh):
    specs_in = (P("data", None), P(None, "data", None), P(), P(), P(), P(), P(), P(), P())
    specs_out = (P(), P(), P(), P(), P(), P(), P())
    return jax.shard_map(local_step, mesh=mesh, in_specs=specs_in, out_specs=specs_out, check_vma=False)
```

```python
import functools

import jax
import jax.numpy as jnp
import numpy as np
from jax import lax
from jax.experimental import pallas as pl
from jax.experimental.pallas import tpu as pltpu
from jax.sharding import PartitionSpec as P

SUB_COUNT = 4
ND = 16
ROWS = 512
WIDTH = 384
FFN = 1536
BATCH = ROWS * ND
CHUNK = 2 * ROWS
BLOCKS = 17
HALF_ROWS = BLOCKS * WIDTH // 2
PART_ROWS = HALF_ROWS // 3
PIECE = PART_ROWS // 8
PARTS = range(3)
NEAR, FAR = range(3, -1, -1), range(7, 3, -1)
HOPS = (4, 2, 1, 8)
COLS = 512
TILES = range(FFN // COLS)
MESH = pl.DeviceIdType.MESH
VMEM_MAX = 67_043_328
F32, BF16 = jnp.float32, jnp.bfloat16
K0 = float(np.sqrt(2.0 / np.pi).astype(np.float32))
LOW = -3.0e38
LOG2E = float(1.0 / np.log(2.0))

LAST = (((1,), (1,)), ((), ()))
FIRST = (((0,), (0,)), ((), ()))
NORMAL = (((1,), (0,)), ((), ()))


def mm(a, b, dims=NORMAL):
    return lax.dot_general(a, b, dims, preferred_element_type=F32)


def gelu(a):
    return a * (0.5 * (1.0 + jnp.tanh(K0 * (a + 0.044715 * (a * a * a)))))


def gelu_and_slope(a):
    sq = a * a
    t = jnp.tanh(K0 * (a + 0.044715 * (a * sq)))
    cdf = 0.5 * (1.0 + t)
    slope = cdf + a * (0.5 * (1.0 - t * t)) * (K0 + (3.0 * 0.044715 * K0) * sq)
    return a * cdf, slope


def fetches(srcs, dsts, sems):
    pairs = [(srcs[i].at[k], dsts[i].at[k]) for k in range(2) for i in range(2)] + [(srcs[2], dsts[2])]
    return [pltpu.make_async_copy(src, dst, sems.at[i]) for i, (src, dst) in enumerate(pairs)]


def forward_rows(x_ref, y_ref, w1_ref, w2_ref, p_ref, u_ref, loads):
    m = x_ref.shape[0] // SUB_COUNT

    def step(i, _):
        def need(n):
            @pl.when(i == 0)
            def _():
                loads[n].wait()

        at = pl.ds(pl.multiple_of(i * m, m), m)
        h = x_ref[at, :]
        for k in range(2):
            need(2 * k)
            for j in TILES:
                cs = slice(j * COLS, (j + 1) * COLS)
                u_ref[:, cs] = gelu(mm(h, w1_ref[k, :, cs])).astype(BF16)
            need(2 * k + 1)
            h = (h.astype(F32) + mm(u_ref[...], w2_ref[k])).astype(BF16)
        need(4)
        y_ref[at, :] = mm(h, p_ref[...]).astype(BF16)
        return 0

    lax.fori_loop(0, SUB_COUNT, step, 0)


WEIGHTS = [
    pltpu.VMEM((2, WIDTH, FFN), BF16), pltpu.VMEM((2, FFN, WIDTH), BF16), pltpu.VMEM((WIDTH, WIDTH), BF16),
    pltpu.SemaphoreType.DMA((5,))]
INNER, OUTER = pl.BlockSpec(memory_space=pltpu.VMEM), pl.BlockSpec(memory_space=pltpu.HBM)
SCALAR = pl.BlockSpec(memory_space=pltpu.SMEM)


def forward_kernel(x_ref, w1_ref, w2_ref, p_ref, y_ref, u_ref, w1, w2, p, w_sems):
    loads = fetches((w1_ref, w2_ref, p_ref), (w1, w2, p), w_sems)
    for load in loads:
        load.start()
    forward_rows(x_ref, y_ref, w1, w2, p, u_ref, loads)


def tower_forward(rows, w1, w2, p):
    return pl.pallas_call(
        forward_kernel,
        out_shape=jax.ShapeDtypeStruct(rows.shape, BF16),
        in_specs=[INNER] + [OUTER] * 3,
        out_specs=INNER,
        scratch_shapes=[pltpu.VMEM((rows.shape[0] // SUB_COUNT, FFN), BF16)] + WEIGHTS,
        compiler_params=pltpu.CompilerParams(vmem_limit_bytes=VMEM_MAX),
        name="tower_forward",
    )(rows, w1, w2, p)


def backward_rows(x, g, w1_ref, w2_ref, p_ref, add, u_ref, s_ref, h_ref, dl_ref, middle=None):
    h_ref[0] = x
    for k in range(2):
        h = h_ref[k]
        for c in TILES:
            cs = slice(c * COLS, (c + 1) * COLS)
            act, slope = gelu_and_slope(mm(h, w1_ref[k, :, cs]))
            u_ref[k, :, cs] = act.astype(BF16)
            s_ref[k, :, cs] = slope
        h_ref[k + 1] = (h.astype(F32) + mm(u_ref[k], w2_ref[k])).astype(BF16)
    if middle is not None:
        middle()
    add(16, mm(h_ref[2], g, FIRST))
    e = mm(g, p_ref[...], LAST)
    for k in (1, 0):
        eb = e.astype(BF16)
        for c in range(4):
            add(8 + 4 * k + c, mm(u_ref[k, :, c * WIDTH:(c + 1) * WIDTH], eb, FIRST))
        for c in TILES:
            cs = slice(c * COLS, (c + 1) * COLS)
            dl_ref[:, cs] = (s_ref[k, :, cs] * mm(eb, w2_ref[k, cs, :], LAST)).astype(BF16)
        for c in range(2):
            part = mm(h_ref[k], dl_ref[:, 2 * c * WIDTH:2 * (c + 1) * WIDTH], FIRST)
            add(4 * k + 2 * c, part[:, :WIDTH])
            add(4 * k + 2 * c + 1, part[:, WIDTH:])
        if k == 1:
            e = e + mm(dl_ref[...], w1_ref[k], LAST)


def unpack_kernel(q_ref, d_ref, *refs):
    outs, hold, load, store = refs[:6], refs[6], refs[7], refs[8]

    def place(j):
        w1, w2, p = outs[3 * (j // BLOCKS):3 * (j // BLOCKS) + 3]
        n = j % BLOCKS
        if n < 8:
            return w1.at[n // 4, :, pl.ds(n % 4 * WIDTH, WIDTH)]
        if n < 16:
            return w2.at[(n - 8) // 4, pl.ds(n % 4 * WIDTH, WIDTH), :]
        return p

    def fetch(j):
        return pltpu.make_async_copy((q_ref, d_ref)[j // BLOCKS].at[j % BLOCKS], hold.at[j], load.at[j])

    def put(j):
        return pltpu.make_async_copy(hold.at[j], place(j), store.at[j])

    for j in range(2 * BLOCKS):
        fetch(j).start()
    for j in range(2 * BLOCKS):
        fetch(j).wait()
        put(j).start()
    for j in range(2 * BLOCKS):
        put(j).wait()


def unpack(q_blocks, d_blocks, shapes):
    return pl.pallas_call(
        unpack_kernel,
        out_shape=[jax.ShapeDtypeStruct(a, F32) for a in shapes],
        in_specs=[OUTER, OUTER],
        out_specs=[OUTER] * 6,
        scratch_shapes=[
            pltpu.VMEM((2 * BLOCKS, WIDTH, WIDTH), F32),
            pltpu.SemaphoreType.DMA((2 * BLOCKS,)),
            pltpu.SemaphoreType.DMA((2 * BLOCKS,)),
        ],
        compiler_params=pltpu.CompilerParams(vmem_limit_bytes=VMEM_MAX),
        name="unpack",
    )(q_blocks, d_blocks)


def bit_of(me, b):
    return lax.rem(me // (1 << b), 2)


def across(me, b):
    return me + (1 - 2 * bit_of(me, b)) * (1 << b)


def sum_places(me):
    core, bits = bit_of(me, 0), [bit_of(me, b) for b in (1, 2, 3)]
    mine, partner = [], []
    for p in PARTS:
        side = [(bits[(p + i) % 3] * (4 >> i) * PIECE, (1 - bits[(p + i) % 3]) * (4 >> i) * PIECE) for i in range(3)]
        for r in range(8):
            at = p * PART_ROWS + side[0][r >> 2] + side[1][(r >> 1) & 1] + side[2][r & 1]
            mine.append(pl.ds(pl.multiple_of(core * HALF_ROWS + at, 8), PIECE))
            partner.append(pl.ds(pl.multiple_of((1 - core) * HALF_ROWS + at, 8), PIECE))
    return mine, partner, [across(me, b) for b in range(4)]


class Gather:
    def __init__(self, copy):
        self.copy = copy

    def begin(self):
        for level in (2, 1, 0, 3):
            for p in PARTS:
                self.copy(p, 0, level).start()

    def pass_on(self, level, *rs):
        for r in rs:
            for p in PARTS:
                self.copy(p, r, level, True).wait_recv()
                for lower in (*range(level - 1, -1, -1), 3):
                    self.copy(p, r + HOPS[level], lower).start()

    def core(self, *rs):
        for r in rs:
            for p in PARTS:
                self.copy(p, r, 3, True).wait_recv()

    def drain(self):
        for level, n in enumerate(HOPS):
            for r in range(n):
                for p in PARTS:
                    self.copy(p, r, level).wait_send()


def place(me, part, r, other=0):
    dev = across(me, 0) if other else me
    for i in range(3):
        if (r >> (2 - i)) & 1:
            dev = dev + (1 - 2 * bit_of(me, 1 + (part + i) % 3)) * (1 << (1 + (part + i) % 3))
    return dev


def hop(me, own, everyone, cuts, sem, part, r, level, theirs=False):
    n = HOPS[level]
    ss, rs = sem[2 * level], sem[2 * level + 1]
    rows, lo, hi = own.shape[0], cuts[part], cuts[part + 1]

    def at(dev):
        return pl.ds(pl.multiple_of(dev * rows + lo, 16), hi - lo)

    if theirs:
        src = dst = everyone.at[at(place(me, part, r, 1) if level == 3 else place(me, part, r + n))]
    else:
        dst = everyone.at[at(place(me, part, r))]
        src = own.at[pl.ds(lo, hi - lo)] if r == 0 else dst
    return pltpu.make_async_remote_copy(
        src_ref=src, dst_ref=dst, send_sem=ss.at[n * part + r], recv_sem=rs.at[n * part + r],
        device_id=(across(me, 0 if level == 3 else 1 + (part + level) % 3),), device_id_type=MESH)


HOP_SEMS = [pltpu.SemaphoreType.DMA((3 * n,)) for n in HOPS for _ in range(2)]


class DeviceSum:
    def __init__(self, places, own, other, out, bufs, sems, load=None):
        self.mine, self.partner, self.peers = places
        self.own, self.other, self.out, self.load = own, other, out, load
        self.bufs, self.sems = bufs, sems
        self.gather = Gather(self.back)

    def copy(self, src, dst, level, k, b):
        return pltpu.make_async_remote_copy(
            src_ref=src, dst_ref=dst, send_sem=self.sems[2 * level].at[k], recv_sem=self.sems[2 * level + 1].at[k],
            device_id=(self.peers[b],), device_id_type=MESH)

    def swap(self, p, r):
        return self.copy(self.other(p, r), self.bufs[0].at[8 * p + r], 0, 8 * p + r, 0)

    def link(self, p, r, level):
        n = HOPS[level]
        return self.copy(self.own(p, n + r), self.bufs[1 + level].at[n * p + r], 1 + level, n * p + r, 1 + (p + level) % 3)

    def back(self, p, r, level, theirs=False):
        n = HOPS[level]
        if theirs and level == 3:
            dst = self.out.at[self.partner[8 * p + r]]
        else:
            dst = self.out.at[self.mine[8 * p + (r + n if theirs else r)]]
        src = self.own(p, 0) if r == 0 and not theirs else dst
        return self.copy(src, dst, 4 + level, n * p + r, 0 if level == 3 else 1 + (p + level) % 3)

    def keep(self, p):
        return pltpu.make_async_copy(self.own(p, 0), self.out.at[self.mine[8 * p]], self.sems[16].at[p])

    def plus(self, p, r, *terms):
        ref = self.own(p, r)
        value = ref[...]
        for level, k in terms:
            value = value + self.bufs[level][k]
        ref[...] = value

    def start(self):
        for r in reversed(range(8)):
            for p in PARTS:
                if self.load is not None:
                    self.load(p, r).start()
                self.swap(p, r).start()

    def swapped(self, rs):
        for r in rs:
            for p in PARTS:
                if self.load is not None:
                    self.load(p, r).wait()
                self.swap(p, r).wait_recv()
                self.plus(p, r, (0, 8 * p + r))
                if r >= 4:
                    self.link(p, r - 4, 0).start()

    def second(self, r):
        for p in PARTS:
            self.link(p, r, 0).wait_recv()
            self.plus(p, r, (1, 4 * p + r))
            self.link(p, r - 2, 1).start()

    def third(self):
        for p in PARTS:
            self.link(p, 1, 0).wait_recv()
            self.link(p, 1, 1).wait_recv()
            self.plus(p, 1, (1, 4 * p + 1), (2, 2 * p + 1))
            self.link(p, 0, 2).start()

    def finish(self):
        for p in PARTS:
            self.link(p, 0, 0).wait_recv()
            self.link(p, 0, 1).wait_recv()
            self.link(p, 0, 2).wait_recv()
            self.plus(p, 0, (1, 4 * p), (2, 2 * p), (3, p))
        self.gather.begin()
        for p in PARTS:
            self.keep(p).start()

    def close(self):
        self.gather.core(*range(8))
        self.gather.drain()
        for p in PARTS:
            for r in range(8):
                self.swap(p, r).wait_send()
            for level in PARTS:
                for r in range(HOPS[level]):
                    self.link(p, r, level).wait_send()
            self.keep(p).wait()


SUM_BUFS = [pltpu.VMEM((n, PIECE, WIDTH), F32) for n in (24, 12, 6, 3)]
SUM_SEMS = [pltpu.SemaphoreType.DMA((n,)) for n in (24, 12, 6, 3) for _ in range(2)] + HOP_SEMS + [pltpu.SemaphoreType.DMA((3,))]


def gather_kernel(tau_ref, docs_own, x_ref, w1_ref, w2_ref, p_ref, up_ref, stat_ref, q_ref, docs, e_ref, m_ref, g_ref, acc, u_ref,
                  mine_ref, w1, w2, p_w, w_sems, share_send, share_recv, *d_sems):
    me = lax.axis_index("data")
    loads = fetches((w1_ref, w2_ref, p_ref), (w1, w2, p_w), w_sems)
    for load in loads:
        load.start()
    inv_tau = 1.0 / tau_ref[0]
    c = inv_tau * LOG2E
    scale = inv_tau / BATCH
    barrier = pltpu.get_barrier_semaphore()
    for p in range(1, ND):
        pl.semaphore_signal(barrier, inc=1, device_id=(lax.rem(me + p, ND),), device_id_type=MESH)
    pl.semaphore_wait(barrier, ND - 1)

    doc = Gather(functools.partial(hop, me, docs_own, docs, (0, 336, 672, 1024), d_sems))
    doc.begin()
    docs[pl.ds(pl.multiple_of(me * CHUNK, CHUNK), CHUNK), :] = docs_own[...]
    forward_rows(x_ref, q_ref, w1, w2, p_w, u_ref, loads)
    doc.pass_on(2, 0)
    m_ref[...] = jnp.full_like(m_ref, LOW)
    lane = lax.broadcasted_iota(jnp.int32, (ROWS, 128), 1)

    def device_at(k):
        chip = k // 2
        chip = jnp.where(chip == 3, 4, jnp.where(chip == 4, 3, chip))
        flips = 2 * chip + lax.rem(k, 2)
        return me + sum((1 - 2 * bit_of(me, b)) * (1 << b) * lax.rem(flips // (1 << b), 2) for b in range(4))

    def score(k, carry):
        @pl.when(k == 1)
        def _():
            doc.core(0)

        @pl.when(k == 2)
        def _():
            doc.pass_on(1, 0)
            doc.pass_on(0, 0)

        @pl.when(k == 3)
        def _():
            doc.core(1, 2, 4)

        @pl.when(k == 8)
        def _():
            doc.pass_on(1, 1)
            doc.pass_on(0, 1, 2)

        @pl.when(k == 9)
        def _():
            doc.core(3, 5, 6)

        @pl.when(k == 14)
        def _():
            doc.pass_on(0, 3)

        @pl.when(k == 15)
        def _():
            doc.core(7)

        top, total = carry
        base = device_at(k) * CHUNK
        marks = m_ref[...]
        for half in range(2):
            rows = docs[pl.ds(pl.multiple_of(base + half * ROWS, ROWS), ROWS), :]
            s = mm(q_ref[...], rows, LAST)
            best = jnp.max(s, axis=1, keepdims=True)
            e = jnp.exp2((s - best) * c)
            e_ref[k, :, half * ROWS:(half + 1) * ROWS] = e
            marks = jnp.where(lane == 2 * k + half, best, marks)
            new_top = jnp.maximum(top, best)
            total = total * jnp.exp2((top - new_top) * c) + jnp.sum(e, axis=1, keepdims=True) * jnp.exp2((best - new_top) * c)
            top = new_top
        m_ref[...] = marks
        return top, total

    top, total = lax.fori_loop(0, ND, score, (jnp.full((ROWS, 1), LOW, F32), jnp.zeros((ROWS, 1), F32)))
    pos = jnp.sum(q_ref[...].astype(F32) * docs_own[0:ROWS, :].astype(F32), axis=1, keepdims=True)
    loss = (top - pos) * inv_tau + jnp.log(total)
    weight = scale / total
    mine_ref[...] = jnp.where(lane == 0, top, jnp.where(lane == 1, weight, loss)).T[0:8, :]
    stat_ref[me] = mine_ref[...]

    def share(p, slot):
        return pltpu.make_async_remote_copy(
            src_ref=mine_ref, dst_ref=stat_ref.at[slot], send_sem=share_send.at[p], recv_sem=share_recv.at[p],
            device_id=(lax.rem(me + p, ND),), device_id_type=MESH)

    for p in range(1, ND):
        share(p, me).start()
    m_ref[...] = jnp.exp2((m_ref[...] - top) * c) * weight

    def weighted(k, half):
        f = jnp.sum(jnp.where(lane == 2 * k + half, m_ref[...], 0.0), axis=1, keepdims=True)
        return e_ref[k, :, half * ROWS:(half + 1) * ROWS] * f

    r = lax.broadcasted_iota(jnp.int32, (ROWS, ROWS), 0)
    col = lax.broadcasted_iota(jnp.int32, (ROWS, ROWS), 1)
    acc[...] = mm((weighted(0, 0) - jnp.where(r == col, scale, 0.0)).astype(BF16), docs_own[0:ROWS, :])
    acc[...] += mm(weighted(0, 1).astype(BF16), docs_own[ROWS:, :])

    def pull(k, _):
        base = device_at(k) * CHUNK
        for half in range(2):
            g_ref[:, half * ROWS:(half + 1) * ROWS] = weighted(k, half).astype(BF16)
        acc[...] += mm(g_ref[...], docs[pl.ds(pl.multiple_of(base, CHUNK), CHUNK), :])
        return 0

    lax.fori_loop(1, ND, pull, 0)
    up_ref[...] = acc[...].astype(BF16)
    for p in range(1, ND):
        share(p, me).wait_send()
        share(p, lax.rem(me + ND - p, ND)).wait_recv()
    doc.drain()


def gather_rows(tau, docs_own, x, w1, w2, p):
    mine = jax.ShapeDtypeStruct((ROWS, WIDTH), BF16)
    return pl.pallas_call(
        gather_kernel,
        out_shape=[mine, jax.ShapeDtypeStruct((ND, 8, ROWS), F32), mine],
        in_specs=[SCALAR, INNER, INNER] + [OUTER] * 3,
        out_specs=[INNER] * 3,
        scratch_shapes=[
            pltpu.VMEM((2 * BATCH, WIDTH), BF16),
            pltpu.VMEM((ND, ROWS, CHUNK), F32),
            pltpu.VMEM((ROWS, 128), F32),
            pltpu.VMEM((ROWS, CHUNK), BF16),
            pltpu.VMEM((ROWS, WIDTH), F32),
            pltpu.VMEM((ROWS // SUB_COUNT, FFN), BF16),
            pltpu.VMEM((8, ROWS), F32),
        ] + WEIGHTS + [pltpu.SemaphoreType.DMA((ND,)), pltpu.SemaphoreType.DMA((ND,))] + HOP_SEMS,
        compiler_params=pltpu.CompilerParams(collective_id=0, has_side_effects=True, vmem_limit_bytes=VMEM_MAX),
        name="gather_rows",
    )(tau, docs_own, x, w1, w2, p)


def greet(peers):
    barrier = pltpu.get_barrier_semaphore()
    for peer in peers:
        pl.semaphore_signal(barrier, inc=1, device_id=(peer,), device_id_type=MESH)
    pl.semaphore_wait(barrier, len(peers))


def query_kernel(q_ref, x_ref, up_ref, w1_ref, w2_ref, p_ref, out_ref, q_all, u_ref, s_ref, h_ref, dl_ref, w1, w2, p, w_sems,
                 local_sem, *sems):
    me = lax.axis_index("data")
    loads = fetches((w1_ref, w2_ref, p_ref), (w1, w2, p), w_sems)
    for load in loads:
        load.start()
    greet([across(me, b) for b in range(4)])
    qry = Gather(functools.partial(hop, me, q_ref, q_all, (0, 176, 352, 512), sems))
    qry.begin()
    local = pltpu.make_async_copy(q_ref, q_all.at[pl.ds(pl.multiple_of(me * ROWS, ROWS), ROWS)], local_sem)
    local.start()
    out_ref[...] = jnp.zeros_like(out_ref)
    for load in loads:
        load.wait()
    m = ROWS // SUB_COUNT

    def add(block, value):
        out_ref[block * WIDTH:(block + 1) * WIDTH, :] += value

    def step(i, _):
        @pl.when(i == 1)
        def _():
            qry.pass_on(2, 0)

        @pl.when(i == 2)
        def _():
            qry.pass_on(1, 0)
            qry.pass_on(0, 0)

        @pl.when(i == 3)
        def _():
            qry.pass_on(1, 1)

        at = pl.ds(pl.multiple_of(i * m, m), m)
        backward_rows(x_ref[at, :], up_ref[at, :], w1, w2, p, add, u_ref, s_ref, h_ref, dl_ref)
        return 0

    lax.fori_loop(0, SUB_COUNT, step, 0)
    qry.pass_on(0, 1, 2, 3)
    qry.core(*range(8))
    qry.drain()
    local.wait()


def backward_scratch(m):
    return [pltpu.VMEM((2, m, FFN), BF16), pltpu.VMEM((2, m, FFN), F32), pltpu.VMEM((3, m, WIDTH), BF16), pltpu.VMEM((m, FFN), BF16)]


PACKED = jax.ShapeDtypeStruct((BLOCKS * WIDTH, WIDTH), F32)


def query_backward(q, x, up, w1, w2, p):
    return pl.pallas_call(
        query_kernel,
        out_shape=[PACKED, jax.ShapeDtypeStruct((BATCH, WIDTH), BF16)],
        in_specs=[INNER] * 3 + [OUTER] * 3,
        out_specs=[INNER, OUTER],
        scratch_shapes=backward_scratch(ROWS // SUB_COUNT) + WEIGHTS + [pltpu.SemaphoreType.DMA] + HOP_SEMS,
        compiler_params=pltpu.CompilerParams(collective_id=2, has_side_effects=True, vmem_limit_bytes=VMEM_MAX),
        name="query_backward",
    )(q, x, up, w1, w2, p)


def tail_kernel(tau_ref, stat_ref, own_ref, x_ref, w1_ref, w2_ref, p_ref, grads_q, q_ref, out_q, out_d,
                q_buf, g_ref, up_ref, grads, u_ref, s_ref, h_ref, dl_ref, w1, w2, p_w, w_sems, held, q_sem, load_sems, *rest):
    me = lax.axis_index("data")
    loads = fetches((w1_ref, w2_ref, p_ref), (w1, w2, p_w), w_sems)
    inv_tau = 1.0 / tau_ref[0]
    c = inv_tau * LOG2E
    scale = inv_tau / BATCH
    places = mine, partner, peers = sum_places(me)
    greet(peers)
    queries = pltpu.make_async_copy(q_ref, q_buf, q_sem)

    def load(p, r):
        k = 8 * p + r
        return pltpu.make_async_copy(grads_q.at[mine[k]], held.at[k], load_sems.at[k])

    sum_q = DeviceSum(places, lambda p, r: held.at[8 * p + r], lambda p, r: grads_q.at[partner[8 * p + r]], out_q,
                      rest[0:4], rest[8:25], load)
    sum_d = DeviceSum(places, lambda p, r: grads.at[mine[8 * p + r]], lambda p, r: grads.at[partner[8 * p + r]], out_d,
                      rest[4:8], rest[25:42])
    sum_q.start()
    queries.start()
    for load in loads:
        load.start()
    sum_q.swapped(FAR)

    def rows_of(k):
        return pl.ds(pl.multiple_of(lax.rem(me + k, ND) * ROWS, ROWS), ROWS)

    def probs(k):
        j = lax.rem(me + k, ND)
        s = mm(own_ref[...], q_buf[rows_of(k), :], LAST)
        return jnp.exp2((s - stat_ref[j, 0:1, :]) * c) * stat_ref[j, 1:2, :]

    grads[...] = jnp.zeros_like(grads)
    queries.wait()
    row = lax.broadcasted_iota(jnp.int32, (CHUNK, ROWS), 0)
    col = lax.broadcasted_iota(jnp.int32, (CHUNK, ROWS), 1)
    up_ref[...] = mm((probs(0) - jnp.where(row == col, scale, 0.0)).astype(BF16), q_buf[rows_of(0), :])

    def columns(i, _):
        @pl.when(i == 1)
        def _():
            sum_q.swapped(NEAR)

        @pl.when(i == 2)
        def _():
            sum_q.second(3)

        @pl.when(i == 3)
        def _():
            sum_q.second(2)

        for n in range(3):
            k = 3 * i + n + 1
            g_ref[n % 2] = probs(k).astype(BF16)
            up_ref[...] += mm(g_ref[n % 2], q_buf[rows_of(k), :])
        return 0

    lax.fori_loop(0, 5, columns, 0)
    for load in loads:
        load.wait()
    m = CHUNK // SUB_COUNT

    def add(block, value):
        grads[block * WIDTH:(block + 1) * WIDTH, :] += value

    def backward(i, _):
        @pl.when(i == 2)
        def _():
            sum_q.finish()

        @pl.when(i == 3)
        def _():
            sum_q.gather.pass_on(2, 0)

        def middle():
            @pl.when(i == 0)
            def _():
                sum_q.third()

        at = pl.ds(pl.multiple_of(i * m, m), m)
        backward_rows(x_ref[at, :], up_ref[at, :].astype(BF16), w1, w2, p_w, add, u_ref, s_ref, h_ref, dl_ref, middle)
        return 0

    lax.fori_loop(0, SUB_COUNT, backward, 0)
    sum_d.start()
    sum_q.gather.pass_on(1, 0)
    sum_d.swapped(FAR)
    sum_q.gather.pass_on(1, 1)
    sum_d.swapped(NEAR)
    sum_q.gather.pass_on(0, 0, 1)
    sum_d.second(3)
    sum_q.gather.pass_on(0, 2)
    sum_d.second(2)
    sum_q.gather.pass_on(0, 3)
    sum_d.third()
    sum_d.finish()
    sum_d.gather.pass_on(2, 0)
    sum_d.gather.pass_on(1, 0, 1)
    sum_d.gather.pass_on(0, *range(4))
    sum_q.close()
    sum_d.close()


def tail(tau, stats, own, x, w1, w2, p, grads_q, q_all):
    return pl.pallas_call(
        tail_kernel,
        out_shape=[PACKED, PACKED],
        in_specs=[SCALAR] + [INNER] * 3 + [OUTER] * 5,
        out_specs=[OUTER, OUTER],
        scratch_shapes=[
            pltpu.VMEM((BATCH, WIDTH), BF16),
            pltpu.VMEM((2, CHUNK, ROWS), BF16),
            pltpu.VMEM((CHUNK, WIDTH), F32),
            pltpu.VMEM(PACKED.shape, F32),
        ] + backward_scratch(CHUNK // SUB_COUNT) + WEIGHTS + [
            pltpu.VMEM((24, PIECE, WIDTH), F32),
            pltpu.SemaphoreType.DMA,
            pltpu.SemaphoreType.DMA((24,)),
        ] + SUM_BUFS + SUM_BUFS + SUM_SEMS + SUM_SEMS,
        compiler_params=pltpu.CompilerParams(collective_id=1, has_side_effects=True, vmem_limit_bytes=VMEM_MAX),
        name="tail",
    )(tau, stats, own, x, w1, w2, p, grads_q, q_all)


def local_step(q_loc, d_loc, temperature, q_w1, q_w2, q_proj, d_w1, d_w2, d_proj):
    tau = temperature.reshape(1)
    d_rows = d_loc.reshape(CHUNK, WIDTH)
    d_reps = tower_forward(d_rows, d_w1, d_w2, d_proj)
    q_up, stats, q_reps = gather_rows(tau, d_reps, q_loc, q_w1, q_w2, q_proj)
    loss = jnp.sum(stats[:, 2, :]) / BATCH
    q_grads, q_all = query_backward(q_reps, q_loc, q_up, q_w1, q_w2, q_proj)
    q_sum, d_sum = tail(tau, stats, d_reps, d_rows, d_w1, d_w2, d_proj, q_grads, q_all)
    shapes = [a.shape for a in (q_w1, q_w2, q_proj, d_w1, d_w2, d_proj)]
    packed = (BLOCKS, WIDTH, WIDTH)
    return (loss, *unpack(q_sum.reshape(packed), d_sum.reshape(packed), shapes))


def solution(mesh):
    specs_in = (P("data", None), P(None, "data", None), P(), P(), P(), P(), P(), P(), P())
    specs_out = (P(), P(), P(), P(), P(), P(), P())
    return jax.shard_map(local_step, mesh=mesh, in_specs=specs_in, out_specs=specs_out, check_vma=False)
```

```python
import functools

import jax
import jax.numpy as jnp
import numpy as np
from jax import lax
from jax.experimental import pallas as pl
from jax.experimental.pallas import tpu as pltpu
from jax.sharding import PartitionSpec as P

SUB_COUNT = 4
ND = 16
ROWS = 512
WIDTH = 384
FFN = 1536
BATCH = ROWS * ND
CHUNK = 2 * ROWS
BLOCKS = 17
HALF_ROWS = BLOCKS * WIDTH // 2
PART_ROWS = HALF_ROWS // 3
PIECE = PART_ROWS // 8
PARTS = range(3)
NEAR, FAR = range(3, -1, -1), range(7, 3, -1)
HOPS = (4, 2, 1, 8)
COLS = 512
TILES = range(FFN // COLS)
MESH = pl.DeviceIdType.MESH
VMEM_MAX = 67_043_328
F32, BF16 = jnp.float32, jnp.bfloat16
K0 = float(np.sqrt(2.0 / np.pi).astype(np.float32))
LOW = -3.0e38
LOG2E = float(1.0 / np.log(2.0))

LAST = (((1,), (1,)), ((), ()))
FIRST = (((0,), (0,)), ((), ()))
NORMAL = (((1,), (0,)), ((), ()))


def mm(a, b, dims=NORMAL):
    return lax.dot_general(a, b, dims, preferred_element_type=F32)


def gelu(a):
    return a * (0.5 * (1.0 + jnp.tanh(K0 * (a + 0.044715 * (a * a * a)))))


def gelu_and_slope(a):
    sq = a * a
    t = jnp.tanh(K0 * (a + 0.044715 * (a * sq)))
    cdf = 0.5 * (1.0 + t)
    slope = cdf + a * (0.5 * (1.0 - t * t)) * (K0 + (3.0 * 0.044715 * K0) * sq)
    return a * cdf, slope


def fetches(srcs, dsts, sems):
    pairs = [(srcs[i].at[k], dsts[i].at[k]) for k in range(2) for i in range(2)] + [(srcs[2], dsts[2])]
    return [pltpu.make_async_copy(src, dst, sems.at[i]) for i, (src, dst) in enumerate(pairs)]


def forward_rows(x_ref, y_ref, w1_ref, w2_ref, p_ref, u_ref, loads):
    m = x_ref.shape[0] // SUB_COUNT
    for load in loads:
        load.wait()

    def step(i, _):
        at = pl.ds(pl.multiple_of(i * m, m), m)
        h = x_ref[at, :]
        for k in range(2):
            for j in TILES:
                cs = slice(j * COLS, (j + 1) * COLS)
                u_ref[:, cs] = gelu(mm(h, w1_ref[k, :, cs])).astype(BF16)
            h = (h.astype(F32) + mm(u_ref[...], w2_ref[k])).astype(BF16)
        y_ref[at, :] = mm(h, p_ref[...]).astype(BF16)
        return 0

    lax.fori_loop(0, SUB_COUNT, step, 0)


WEIGHTS = [
    pltpu.VMEM((2, WIDTH, FFN), BF16), pltpu.VMEM((2, FFN, WIDTH), BF16), pltpu.VMEM((WIDTH, WIDTH), BF16),
    pltpu.SemaphoreType.DMA((5,))]
INNER, OUTER = pl.BlockSpec(memory_space=pltpu.VMEM), pl.BlockSpec(memory_space=pltpu.HBM)
SCALAR = pl.BlockSpec(memory_space=pltpu.SMEM)


def forward_kernel(x_ref, w1_ref, w2_ref, p_ref, y_ref, u_ref, w1, w2, p, w_sems):
    loads = fetches((w1_ref, w2_ref, p_ref), (w1, w2, p), w_sems)
    for load in loads:
        load.start()
    forward_rows(x_ref, y_ref, w1, w2, p, u_ref, loads)


def tower_forward(rows, w1, w2, p):
    return pl.pallas_call(
        forward_kernel,
        out_shape=jax.ShapeDtypeStruct(rows.shape, BF16),
        in_specs=[INNER] + [OUTER] * 3,
        out_specs=INNER,
        scratch_shapes=[pltpu.VMEM((rows.shape[0] // SUB_COUNT, FFN), BF16)] + WEIGHTS,
        compiler_params=pltpu.CompilerParams(vmem_limit_bytes=VMEM_MAX),
        name="tower_forward",
    )(rows, w1, w2, p)


def backward_rows(x, g, w1_ref, w2_ref, p_ref, add, u_ref, s_ref, h_ref, dl_ref, middle=None):
    h_ref[0] = x
    for k in range(2):
        h = h_ref[k]
        for c in TILES:
            cs = slice(c * COLS, (c + 1) * COLS)
            act, slope = gelu_and_slope(mm(h, w1_ref[k, :, cs]))
            u_ref[k, :, cs] = act.astype(BF16)
            s_ref[k, :, cs] = slope
        h_ref[k + 1] = (h.astype(F32) + mm(u_ref[k], w2_ref[k])).astype(BF16)
    if middle is not None:
        middle()
    add(16, mm(h_ref[2], g, FIRST))
    e = mm(g, p_ref[...], LAST)
    for k in (1, 0):
        eb = e.astype(BF16)
        for c in range(4):
            add(8 + 4 * k + c, mm(u_ref[k, :, c * WIDTH:(c + 1) * WIDTH], eb, FIRST))
        for c in TILES:
            cs = slice(c * COLS, (c + 1) * COLS)
            dl_ref[:, cs] = (s_ref[k, :, cs] * mm(eb, w2_ref[k, cs, :], LAST)).astype(BF16)
        for c in range(2):
            part = mm(h_ref[k], dl_ref[:, 2 * c * WIDTH:2 * (c + 1) * WIDTH], FIRST)
            add(4 * k + 2 * c, part[:, :WIDTH])
            add(4 * k + 2 * c + 1, part[:, WIDTH:])
        if k == 1:
            e = e + mm(dl_ref[...], w1_ref[k], LAST)


def unpack_kernel(q_ref, d_ref, *refs):
    outs, hold, load, store = refs[:6], refs[6], refs[7], refs[8]

    def place(j):
        w1, w2, p = outs[3 * (j // BLOCKS):3 * (j // BLOCKS) + 3]
        n = j % BLOCKS
        if n < 8:
            return w1.at[n // 4, :, pl.ds(n % 4 * WIDTH, WIDTH)]
        if n < 16:
            return w2.at[(n - 8) // 4, pl.ds(n % 4 * WIDTH, WIDTH), :]
        return p

    def fetch(j):
        return pltpu.make_async_copy((q_ref, d_ref)[j // BLOCKS].at[j % BLOCKS], hold.at[j], load.at[j])

    def put(j):
        return pltpu.make_async_copy(hold.at[j], place(j), store.at[j])

    for j in range(2 * BLOCKS):
        fetch(j).start()
    for j in range(2 * BLOCKS):
        fetch(j).wait()
        put(j).start()
    for j in range(2 * BLOCKS):
        put(j).wait()


def unpack(q_blocks, d_blocks, shapes):
    return pl.pallas_call(
        unpack_kernel,
        out_shape=[jax.ShapeDtypeStruct(a, F32) for a in shapes],
        in_specs=[OUTER, OUTER],
        out_specs=[OUTER] * 6,
        scratch_shapes=[
            pltpu.VMEM((2 * BLOCKS, WIDTH, WIDTH), F32),
            pltpu.SemaphoreType.DMA((2 * BLOCKS,)),
            pltpu.SemaphoreType.DMA((2 * BLOCKS,)),
        ],
        compiler_params=pltpu.CompilerParams(vmem_limit_bytes=VMEM_MAX),
        name="unpack",
    )(q_blocks, d_blocks)


def bit_of(me, b):
    return lax.rem(me // (1 << b), 2)


def across(me, b):
    return me + (1 - 2 * bit_of(me, b)) * (1 << b)


def sum_places(me):
    core, bits = bit_of(me, 0), [bit_of(me, b) for b in (1, 2, 3)]
    mine, partner = [], []
    for p in PARTS:
        side = [(bits[(p + i) % 3] * (4 >> i) * PIECE, (1 - bits[(p + i) % 3]) * (4 >> i) * PIECE) for i in range(3)]
        for r in range(8):
            at = p * PART_ROWS + side[0][r >> 2] + side[1][(r >> 1) & 1] + side[2][r & 1]
            mine.append(pl.ds(pl.multiple_of(core * HALF_ROWS + at, 8), PIECE))
            partner.append(pl.ds(pl.multiple_of((1 - core) * HALF_ROWS + at, 8), PIECE))
    return mine, partner, [across(me, b) for b in range(4)]


class Gather:
    def __init__(self, copy):
        self.copy = copy

    def begin(self):
        for level in (2, 1, 0, 3):
            for p in PARTS:
                self.copy(p, 0, level).start()

    def pass_on(self, level, *rs):
        for r in rs:
            for p in PARTS:
                self.copy(p, r, level, True).wait_recv()
                for lower in (*range(level - 1, -1, -1), 3):
                    self.copy(p, r + HOPS[level], lower).start()

    def core(self, *rs):
        for r in rs:
            for p in PARTS:
                self.copy(p, r, 3, True).wait_recv()

    def drain(self):
        for level, n in enumerate(HOPS):
            for r in range(n):
                for p in PARTS:
                    self.copy(p, r, level).wait_send()


def place(me, part, r, other=0):
    dev = across(me, 0) if other else me
    for i in range(3):
        if (r >> (2 - i)) & 1:
            dev = dev + (1 - 2 * bit_of(me, 1 + (part + i) % 3)) * (1 << (1 + (part + i) % 3))
    return dev


def hop(me, own, everyone, cuts, sem, part, r, level, theirs=False):
    n = HOPS[level]
    ss, rs = sem[2 * level], sem[2 * level + 1]
    rows, lo, hi = own.shape[0], cuts[part], cuts[part + 1]

    def at(dev):
        return pl.ds(pl.multiple_of(dev * rows + lo, 16), hi - lo)

    if theirs:
        src = dst = everyone.at[at(place(me, part, r, 1) if level == 3 else place(me, part, r + n))]
    else:
        dst = everyone.at[at(place(me, part, r))]
        src = own.at[pl.ds(lo, hi - lo)] if r == 0 else dst
    return pltpu.make_async_remote_copy(
        src_ref=src, dst_ref=dst, send_sem=ss.at[n * part + r], recv_sem=rs.at[n * part + r],
        device_id=(across(me, 0 if level == 3 else 1 + (part + level) % 3),), device_id_type=MESH)


HOP_SEMS = [pltpu.SemaphoreType.DMA((3 * n,)) for n in HOPS for _ in range(2)]


class DeviceSum:
    def __init__(self, places, own, other, out, bufs, sems, load=None):
        self.mine, self.partner, self.peers = places
        self.own, self.other, self.out, self.load = own, other, out, load
        self.bufs, self.sems = bufs, sems
        self.gather = Gather(self.back)

    def copy(self, src, dst, level, k, b):
        return pltpu.make_async_remote_copy(
            src_ref=src, dst_ref=dst, send_sem=self.sems[2 * level].at[k], recv_sem=self.sems[2 * level + 1].at[k],
            device_id=(self.peers[b],), device_id_type=MESH)

    def swap(self, p, r):
        return self.copy(self.other(p, r), self.bufs[0].at[8 * p + r], 0, 8 * p + r, 0)

    def link(self, p, r, level):
        n = HOPS[level]
        return self.copy(self.own(p, n + r), self.bufs[1 + level].at[n * p + r], 1 + level, n * p + r, 1 + (p + level) % 3)

    def back(self, p, r, level, theirs=False):
        n = HOPS[level]
        if theirs and level == 3:
            dst = self.out.at[self.partner[8 * p + r]]
        else:
            dst = self.out.at[self.mine[8 * p + (r + n if theirs else r)]]
        src = self.own(p, 0) if r == 0 and not theirs else dst
        return self.copy(src, dst, 4 + level, n * p + r, 0 if level == 3 else 1 + (p + level) % 3)

    def keep(self, p):
        return pltpu.make_async_copy(self.own(p, 0), self.out.at[self.mine[8 * p]], self.sems[16].at[p])

    def plus(self, p, r, *terms):
        ref = self.own(p, r)
        value = ref[...]
        for level, k in terms:
            value = value + self.bufs[level][k]
        ref[...] = value

    def start(self):
        for r in reversed(range(8)):
            for p in PARTS:
                if self.load is not None:
                    self.load(p, r).start()
                self.swap(p, r).start()

    def swapped(self, rs):
        for r in rs:
            for p in PARTS:
                if self.load is not None:
                    self.load(p, r).wait()
                self.swap(p, r).wait_recv()
                self.plus(p, r, (0, 8 * p + r))
                if r >= 4:
                    self.link(p, r - 4, 0).start()

    def second(self, r):
        for p in PARTS:
            self.link(p, r, 0).wait_recv()
            self.plus(p, r, (1, 4 * p + r))
            self.link(p, r - 2, 1).start()

    def third(self):
        for p in PARTS:
            self.link(p, 1, 0).wait_recv()
            self.link(p, 1, 1).wait_recv()
            self.plus(p, 1, (1, 4 * p + 1), (2, 2 * p + 1))
            self.link(p, 0, 2).start()

    def finish(self):
        for p in PARTS:
            self.link(p, 0, 0).wait_recv()
            self.link(p, 0, 1).wait_recv()
            self.link(p, 0, 2).wait_recv()
            self.plus(p, 0, (1, 4 * p), (2, 2 * p), (3, p))
        self.gather.begin()
        for p in PARTS:
            self.keep(p).start()

    def close(self):
        self.gather.core(*range(8))
        self.gather.drain()
        for p in PARTS:
            for r in range(8):
                self.swap(p, r).wait_send()
            for level in PARTS:
                for r in range(HOPS[level]):
                    self.link(p, r, level).wait_send()
            self.keep(p).wait()


SUM_BUFS = [pltpu.VMEM((n, PIECE, WIDTH), F32) for n in (24, 12, 6, 3)]
SUM_SEMS = [pltpu.SemaphoreType.DMA((n,)) for n in (24, 12, 6, 3) for _ in range(2)] + HOP_SEMS + [pltpu.SemaphoreType.DMA((3,))]


def gather_kernel(tau_ref, docs_own, x_ref, w1_ref, w2_ref, p_ref, up_ref, stat_ref, q_ref, docs, e_ref, m_ref, g_ref, acc, u_ref,
                  mine_ref, w1, w2, p_w, w_sems, share_send, share_recv, *d_sems):
    me = lax.axis_index("data")
    loads = fetches((w1_ref, w2_ref, p_ref), (w1, w2, p_w), w_sems)
    for load in loads:
        load.start()
    inv_tau = 1.0 / tau_ref[0]
    c = inv_tau * LOG2E
    scale = inv_tau / BATCH
    barrier = pltpu.get_barrier_semaphore()
    for p in range(1, ND):
        pl.semaphore_signal(barrier, inc=1, device_id=(lax.rem(me + p, ND),), device_id_type=MESH)
    pl.semaphore_wait(barrier, ND - 1)

    doc = Gather(functools.partial(hop, me, docs_own, docs, (0, 336, 672, 1024), d_sems))
    doc.begin()
    docs[pl.ds(pl.multiple_of(me * CHUNK, CHUNK), CHUNK), :] = docs_own[...]
    forward_rows(x_ref, q_ref, w1, w2, p_w, u_ref, loads)
    doc.pass_on(2, 0)
    m_ref[...] = jnp.full_like(m_ref, LOW)
    lane = lax.broadcasted_iota(jnp.int32, (ROWS, 128), 1)

    def device_at(k):
        chip = k // 2
        chip = jnp.where(chip == 3, 4, jnp.where(chip == 4, 3, chip))
        flips = 2 * chip + lax.rem(k, 2)
        return me + sum((1 - 2 * bit_of(me, b)) * (1 << b) * lax.rem(flips // (1 << b), 2) for b in range(4))

    def score(k, carry):
        @pl.when(k == 1)
        def _():
            doc.core(0)

        @pl.when(k == 2)
        def _():
            doc.pass_on(1, 0)
            doc.pass_on(0, 0)

        @pl.when(k == 3)
        def _():
            doc.core(1, 2, 4)

        @pl.when(k == 8)
        def _():
            doc.pass_on(1, 1)
            doc.pass_on(0, 1, 2)

        @pl.when(k == 9)
        def _():
            doc.core(3, 5, 6)

        @pl.when(k == 14)
        def _():
            doc.pass_on(0, 3)

        @pl.when(k == 15)
        def _():
            doc.core(7)

        top, total = carry
        base = device_at(k) * CHUNK
        marks = m_ref[...]
        for half in range(2):
            rows = docs[pl.ds(pl.multiple_of(base + half * ROWS, ROWS), ROWS), :]
            s = mm(q_ref[...], rows, LAST)
            best = jnp.max(s, axis=1, keepdims=True)
            e = jnp.exp2((s - best) * c)
            e_ref[k, :, half * ROWS:(half + 1) * ROWS] = e
            marks = jnp.where(lane == 2 * k + half, best, marks)
            new_top = jnp.maximum(top, best)
            total = total * jnp.exp2((top - new_top) * c) + jnp.sum(e, axis=1, keepdims=True) * jnp.exp2((best - new_top) * c)
            top = new_top
        m_ref[...] = marks
        return top, total

    top, total = lax.fori_loop(0, ND, score, (jnp.full((ROWS, 1), LOW, F32), jnp.zeros((ROWS, 1), F32)))
    pos = jnp.sum(q_ref[...].astype(F32) * docs_own[0:ROWS, :].astype(F32), axis=1, keepdims=True)
    loss = (top - pos) * inv_tau + jnp.log(total)
    weight = scale / total
    mine_ref[...] = jnp.where(lane == 0, top, jnp.where(lane == 1, weight, loss)).T[0:8, :]
    stat_ref[me] = mine_ref[...]

    def share(p, slot):
        return pltpu.make_async_remote_copy(
            src_ref=mine_ref, dst_ref=stat_ref.at[slot], send_sem=share_send.at[p], recv_sem=share_recv.at[p],
            device_id=(lax.rem(me + p, ND),), device_id_type=MESH)

    for p in range(1, ND):
        share(p, me).start()
    m_ref[...] = jnp.exp2((m_ref[...] - top) * c) * weight

    def weighted(k, half):
        f = jnp.sum(jnp.where(lane == 2 * k + half, m_ref[...], 0.0), axis=1, keepdims=True)
        return e_ref[k, :, half * ROWS:(half + 1) * ROWS] * f

    r = lax.broadcasted_iota(jnp.int32, (ROWS, ROWS), 0)
    col = lax.broadcasted_iota(jnp.int32, (ROWS, ROWS), 1)
    acc[...] = mm((weighted(0, 0) - jnp.where(r == col, scale, 0.0)).astype(BF16), docs_own[0:ROWS, :])
    acc[...] += mm(weighted(0, 1).astype(BF16), docs_own[ROWS:, :])

    def pull(k, _):
        base = device_at(k) * CHUNK
        for half in range(2):
            g_ref[:, half * ROWS:(half + 1) * ROWS] = weighted(k, half).astype(BF16)
        acc[...] += mm(g_ref[...], docs[pl.ds(pl.multiple_of(base, CHUNK), CHUNK), :])
        return 0

    lax.fori_loop(1, ND, pull, 0)
    up_ref[...] = acc[...].astype(BF16)
    for p in range(1, ND):
        share(p, me).wait_send()
        share(p, lax.rem(me + ND - p, ND)).wait_recv()
    doc.drain()


def gather_rows(tau, docs_own, x, w1, w2, p):
    mine = jax.ShapeDtypeStruct((ROWS, WIDTH), BF16)
    return pl.pallas_call(
        gather_kernel,
        out_shape=[mine, jax.ShapeDtypeStruct((ND, 8, ROWS), F32), mine],
        in_specs=[SCALAR, INNER, INNER] + [OUTER] * 3,
        out_specs=[INNER] * 3,
        scratch_shapes=[
            pltpu.VMEM((2 * BATCH, WIDTH), BF16),
            pltpu.VMEM((ND, ROWS, CHUNK), F32),
            pltpu.VMEM((ROWS, 128), F32),
            pltpu.VMEM((ROWS, CHUNK), BF16),
            pltpu.VMEM((ROWS, WIDTH), F32),
            pltpu.VMEM((ROWS // SUB_COUNT, FFN), BF16),
            pltpu.VMEM((8, ROWS), F32),
        ] + WEIGHTS + [pltpu.SemaphoreType.DMA((ND,)), pltpu.SemaphoreType.DMA((ND,))] + HOP_SEMS,
        compiler_params=pltpu.CompilerParams(collective_id=0, has_side_effects=True, vmem_limit_bytes=VMEM_MAX),
        name="gather_rows",
    )(tau, docs_own, x, w1, w2, p)


def greet(peers):
    barrier = pltpu.get_barrier_semaphore()
    for peer in peers:
        pl.semaphore_signal(barrier, inc=1, device_id=(peer,), device_id_type=MESH)
    pl.semaphore_wait(barrier, len(peers))


def query_kernel(q_ref, x_ref, up_ref, w1_ref, w2_ref, p_ref, out_ref, q_all, u_ref, s_ref, h_ref, dl_ref, w1, w2, p, w_sems,
                 local_sem, *sems):
    me = lax.axis_index("data")
    loads = fetches((w1_ref, w2_ref, p_ref), (w1, w2, p), w_sems)
    for load in loads:
        load.start()
    greet([across(me, b) for b in range(4)])
    qry = Gather(functools.partial(hop, me, q_ref, q_all, (0, 176, 352, 512), sems))
    qry.begin()
    local = pltpu.make_async_copy(q_ref, q_all.at[pl.ds(pl.multiple_of(me * ROWS, ROWS), ROWS)], local_sem)
    local.start()
    out_ref[...] = jnp.zeros_like(out_ref)
    for load in loads:
        load.wait()
    m = ROWS // SUB_COUNT

    def add(block, value):
        out_ref[block * WIDTH:(block + 1) * WIDTH, :] += value

    def step(i, _):
        @pl.when(i == 1)
        def _():
            qry.pass_on(2, 0)

        @pl.when(i == 2)
        def _():
            qry.pass_on(1, 0)
            qry.pass_on(0, 0)

        @pl.when(i == 3)
        def _():
            qry.pass_on(1, 1)

        at = pl.ds(pl.multiple_of(i * m, m), m)
        backward_rows(x_ref[at, :], up_ref[at, :], w1, w2, p, add, u_ref, s_ref, h_ref, dl_ref)
        return 0

    lax.fori_loop(0, SUB_COUNT, step, 0)
    qry.pass_on(0, 1, 2, 3)
    qry.core(*range(8))
    qry.drain()
    local.wait()


def backward_scratch(m):
    return [pltpu.VMEM((2, m, FFN), BF16), pltpu.VMEM((2, m, FFN), F32), pltpu.VMEM((3, m, WIDTH), BF16), pltpu.VMEM((m, FFN), BF16)]


PACKED = jax.ShapeDtypeStruct((BLOCKS * WIDTH, WIDTH), F32)


def query_backward(q, x, up, w1, w2, p):
    return pl.pallas_call(
        query_kernel,
        out_shape=[PACKED, jax.ShapeDtypeStruct((BATCH, WIDTH), BF16)],
        in_specs=[INNER] * 3 + [OUTER] * 3,
        out_specs=[INNER, OUTER],
        scratch_shapes=backward_scratch(ROWS // SUB_COUNT) + WEIGHTS + [pltpu.SemaphoreType.DMA] + HOP_SEMS,
        compiler_params=pltpu.CompilerParams(collective_id=2, has_side_effects=True, vmem_limit_bytes=VMEM_MAX),
        name="query_backward",
    )(q, x, up, w1, w2, p)


def tail_kernel(tau_ref, stat_ref, own_ref, x_ref, w1_ref, w2_ref, p_ref, grads_q, q_ref, out_q, out_d,
                q_buf, g_ref, up_ref, grads, u_ref, s_ref, h_ref, dl_ref, w1, w2, p_w, w_sems, held, q_sem, load_sems, *rest):
    me = lax.axis_index("data")
    loads = fetches((w1_ref, w2_ref, p_ref), (w1, w2, p_w), w_sems)
    inv_tau = 1.0 / tau_ref[0]
    c = inv_tau * LOG2E
    scale = inv_tau / BATCH
    places = mine, partner, peers = sum_places(me)
    greet(peers)
    queries = pltpu.make_async_copy(q_ref, q_buf, q_sem)

    def load(p, r):
        k = 8 * p + r
        return pltpu.make_async_copy(grads_q.at[mine[k]], held.at[k], load_sems.at[k])

    sum_q = DeviceSum(places, lambda p, r: held.at[8 * p + r], lambda p, r: grads_q.at[partner[8 * p + r]], out_q,
                      rest[0:4], rest[8:25], load)
    sum_d = DeviceSum(places, lambda p, r: grads.at[mine[8 * p + r]], lambda p, r: grads.at[partner[8 * p + r]], out_d,
                      rest[4:8], rest[25:42])
    sum_q.start()
    queries.start()
    for load in loads:
        load.start()
    sum_q.swapped(FAR)

    def rows_of(k):
        return pl.ds(pl.multiple_of(lax.rem(me + k, ND) * ROWS, ROWS), ROWS)

    def probs(k):
        j = lax.rem(me + k, ND)
        s = mm(own_ref[...], q_buf[rows_of(k), :], LAST)
        return jnp.exp2((s - stat_ref[j, 0:1, :]) * c) * stat_ref[j, 1:2, :]

    grads[...] = jnp.zeros_like(grads)
    queries.wait()
    row = lax.broadcasted_iota(jnp.int32, (CHUNK, ROWS), 0)
    col = lax.broadcasted_iota(jnp.int32, (CHUNK, ROWS), 1)
    up_ref[...] = mm((probs(0) - jnp.where(row == col, scale, 0.0)).astype(BF16), q_buf[rows_of(0), :])

    def columns(i, _):
        @pl.when(i == 0)
        def _():
            sum_q.swapped(NEAR)

        @pl.when(i == 1)
        def _():
            sum_q.second(3)

        @pl.when(i == 2)
        def _():
            sum_q.second(2)

        for n in range(3):
            k = 3 * i + n + 1
            g_ref[n % 2] = probs(k).astype(BF16)
            up_ref[...] += mm(g_ref[n % 2], q_buf[rows_of(k), :])
        return 0

    lax.fori_loop(0, 5, columns, 0)
    for load in loads:
        load.wait()
    m = CHUNK // SUB_COUNT

    def add(block, value):
        grads[block * WIDTH:(block + 1) * WIDTH, :] += value

    def backward(i, _):
        def middle():
            @pl.when(i == 0)
            def _():
                sum_q.third()

        @pl.when(i == 1)
        def _():
            sum_q.finish()

        @pl.when(i == 2)
        def _():
            sum_q.gather.pass_on(2, 0)

        @pl.when(i == 3)
        def _():
            sum_q.gather.pass_on(1, 0)

        at = pl.ds(pl.multiple_of(i * m, m), m)
        backward_rows(x_ref[at, :], up_ref[at, :].astype(BF16), w1, w2, p_w, add, u_ref, s_ref, h_ref, dl_ref, middle)
        return 0

    lax.fori_loop(0, SUB_COUNT, backward, 0)
    sum_d.start()
    sum_d.swapped(FAR)
    sum_q.gather.pass_on(0, 0, 1)
    sum_d.swapped(NEAR)
    sum_d.second(3)
    sum_q.gather.pass_on(0, 2)
    sum_d.second(2)
    sum_d.third()
    sum_q.gather.pass_on(1, 1)
    sum_d.finish()
    sum_q.gather.pass_on(0, 3)
    sum_d.gather.pass_on(2, 0)
    sum_d.gather.pass_on(1, 0, 1)
    sum_d.gather.pass_on(0, *range(4))
    sum_q.close()
    sum_d.close()


def tail(tau, stats, own, x, w1, w2, p, grads_q, q_all):
    return pl.pallas_call(
        tail_kernel,
        out_shape=[PACKED, PACKED],
        in_specs=[SCALAR] + [INNER] * 3 + [OUTER] * 5,
        out_specs=[OUTER, OUTER],
        scratch_shapes=[
            pltpu.VMEM((BATCH, WIDTH), BF16),
            pltpu.VMEM((2, CHUNK, ROWS), BF16),
            pltpu.VMEM((CHUNK, WIDTH), F32),
            pltpu.VMEM(PACKED.shape, F32),
        ] + backward_scratch(CHUNK // SUB_COUNT) + WEIGHTS + [
            pltpu.VMEM((24, PIECE, WIDTH), F32),
            pltpu.SemaphoreType.DMA,
            pltpu.SemaphoreType.DMA((24,)),
        ] + SUM_BUFS + SUM_BUFS + SUM_SEMS + SUM_SEMS,
        compiler_params=pltpu.CompilerParams(collective_id=1, has_side_effects=True, vmem_limit_bytes=VMEM_MAX),
        name="tail",
    )(tau, stats, own, x, w1, w2, p, grads_q, q_all)


def local_step(q_loc, d_loc, temperature, q_w1, q_w2, q_proj, d_w1, d_w2, d_proj):
    tau = temperature.reshape(1)
    d_rows = d_loc.reshape(CHUNK, WIDTH)
    d_reps = tower_forward(d_rows, d_w1, d_w2, d_proj)
    q_up, stats, q_reps = gather_rows(tau, d_reps, q_loc, q_w1, q_w2, q_proj)
    loss = jnp.sum(stats[:, 2, :]) / BATCH
    q_grads, q_all = query_backward(q_reps, q_loc, q_up, q_w1, q_w2, q_proj)
    q_sum, d_sum = tail(tau, stats, d_reps, d_rows, d_w1, d_w2, d_proj, q_grads, q_all)
    shapes = [a.shape for a in (q_w1, q_w2, q_proj, d_w1, d_w2, d_proj)]
    packed = (BLOCKS, WIDTH, WIDTH)
    return (loss, *unpack(q_sum.reshape(packed), d_sum.reshape(packed), shapes))


def solution(mesh):
    specs_in = (P("data", None), P(None, "data", None), P(), P(), P(), P(), P(), P(), P())
    specs_out = (P(), P(), P(), P(), P(), P(), P())
    return jax.shard_map(local_step, mesh=mesh, in_specs=specs_in, out_specs=specs_out, check_vma=False)
```
